32 devices in a mesh: zone: 8 (over z, x), freq: 4 (over y, core).
Axes of the slice: x: 2, y: 2, z: 4, core: 2. Of those that a mesh axis runs over, the one named last changes fastest.
Arguments:
- modulus: float32 [64, 3, 1, 1024], P('zone'), may hold values from 0.3 to 1.5
- first_moment: float32 [64, 3, 1, 1024], P('zone'), may hold values from -6 to 6
- second_moment: float32 [64, 3, 1, 1024], P('zone'), may hold values from 0.5 to 4
- fiber: float32 [64, 1, 1024], P('zone'), may hold values from -1 to 1
- measured: float32 [4, 32, 2, 8, 1024], P('freq', 'zone'), may hold values from -6 to 6
- wave_sq: float32 [4], P('freq'), may hold values from 0.5 to 5
- send_list: int32 [8, 8, 2], P('zone'), may hold values from -1 to 7, as said below
- brick_list: int32 [32, 8], P('zone'), may hold values from 0 to 15, as said below
Outputs:
- new_modulus: float32 [64, 3, 1, 1024], P('zone')
- new_first: float32 [64, 3, 1, 1024], P('zone')
- new_second: float32 [64, 3, 1, 1024], P('zone')
The draws below stay inside these ranges and needn't reach their ends.
Inputs may be any that keep to these rules, and one draw needn't show every extreme that they name: `send_list`: entries are -1 or distinct local brick indices; for each owner and zone group the live slots are c < some count of 0 to 2, and owner o sends 2 bricks to group (o + 1) % 8. `brick_list`: every entry names a live slot of its zone group.
All inputs are finite; a program needn't handle non-finite values.
Results may differ from the reference program's by a relative error of at most 0.0001.
Values sent between devices are 32-bit elements; how exact they have to be, the bound alone decides.
No kernel may reach another device: no remote copies, remote signals or barrier semaphores. Data moves between devices by JAX's collectives and lax.ppermute only.
A program may use at most 64 MiB of HBM per device.

```python
import math
import jax
import jax.numpy as jnp
from jax import lax

NB_DEV = 8
SZ_DEV = 4
BX = 1
BY = 32
BZ = 32
K = 8
CAP = 2
SWEEPS = 6
ZGROUPS = 8
FREQS = 4
BRICKS = 64
SUBZONES = 32


def route_tables(key):
    base = jax.random.fold_in(key, 4242)
    key_count = jax.random.fold_in(base, 1)
    key_perm = jax.random.fold_in(base, 2)
    key_pick = jax.random.fold_in(base, 3)
    key_shuffle = jax.random.fold_in(base, 5)
    counts = jax.random.randint(key_count, (ZGROUPS, ZGROUPS), 0, CAP + 1)
    owner_idx = jnp.arange(ZGROUPS, dtype=jnp.int32)[:, None]
    dest_idx = jnp.arange(ZGROUPS, dtype=jnp.int32)[None, :]
    counts = jnp.where(dest_idx == (owner_idx + 1) % ZGROUPS, CAP, counts)
    counts = jnp.where((owner_idx == 0) & (dest_idx == 0), CAP, counts).astype(jnp.int32)
    perm_keys = jax.random.split(key_perm, ZGROUPS * ZGROUPS)
    chosen = jax.vmap(lambda one_key: jax.random.permutation(one_key, NB_DEV)[:CAP])(perm_keys)
    chosen = chosen.reshape(ZGROUPS, ZGROUPS, CAP).astype(jnp.int32)
    chosen = chosen.at[0, 1 % ZGROUPS, 0].set(NB_DEV - 1)
    chosen = chosen.at[0, 1 % ZGROUPS, 1].set(0)
    slot_idx = jnp.arange(CAP, dtype=jnp.int32)[None, None, :]
    live_mask = slot_idx < counts[:, :, None]
    send_table = jnp.where(live_mask, chosen, -1).astype(jnp.int32)
    live_dest = jnp.transpose(live_mask, (1, 0, 2)).reshape(ZGROUPS, ZGROUPS * CAP)
    ordering = jnp.argsort(jnp.where(live_dest, 0, 1).astype(jnp.int32), axis=-1, stable=True).astype(jnp.int32)
    live_total = jnp.sum(live_dest.astype(jnp.int32), axis=-1).astype(jnp.int32)
    entries = SZ_DEV * K
    picks = jax.random.randint(key_pick, (ZGROUPS, entries), 0, live_total[:, None]).astype(jnp.int32)
    seq_idx = jnp.arange(entries, dtype=jnp.int32)[None, :]
    positions = jnp.where(seq_idx < live_total[:, None], seq_idx, picks).astype(jnp.int32)
    shuffle_keys = jax.random.split(key_shuffle, ZGROUPS)
    shuffles = jax.vmap(lambda one_key: jax.random.permutation(one_key, entries))(shuffle_keys).astype(jnp.int32)
    positions = jnp.take_along_axis(positions, shuffles, axis=-1)
    brick_table = jnp.take_along_axis(ordering, positions, axis=-1)
    brick_table = brick_table.reshape(ZGROUPS * SZ_DEV, K).astype(jnp.int32)
    top_slot = (ZGROUPS - 1) * CAP + CAP - 1
    brick_table = brick_table.at[0, 0].set(top_slot)
    brick_table = brick_table.at[0, 1].set(0)
    return (send_table, brick_table.astype(jnp.int32))


def draw_send_list(key, part):
    return route_tables(key)[0]


def draw_brick_list(key, part):
    return route_tables(key)[1]


def shard_levels(own_key, shape, cuts, least, largest):
    loudness, own = 1.0, jax.random.fold_in(own_key, 6)
    for position, blocks in cuts:
        draws = jnp.exp(jax.random.uniform(jax.random.fold_in(own, position), (blocks,), jnp.float32, least / len(cuts), largest / len(cuts)))
        loudness = loudness * jnp.repeat(draws, shape[position] // blocks).reshape([-1 if axis == position else 1 for axis in range(len(shape))])
    return loudness


def gaussian(key, extent, width, reach, cuts=(), held_as=jnp.bfloat16):
    level = shard_levels(key, extent, cuts, -0.22, 0.18) if cuts else 1.0
    values = jax.random.normal(key, extent, jnp.float32) * width * level
    return jnp.minimum(jnp.maximum(values, -reach), reach).astype(held_as)


def setup_inputs(seed: int = 0) -> dict:
    streams_of = jax.random.split(jax.random.key(seed), 9)
    return {
        "modulus": jnp.clip(0.3 + 1.2 * jax.random.uniform(streams_of[0], (BRICKS, 3, BX, BY * BZ), jnp.float32) ** shard_levels(streams_of[0], (BRICKS, 3, BX, BY * BZ), ((0, 8),), -0.2, 0.2), 0.3, 1.5),
        "first_moment": gaussian(streams_of[1], (BRICKS, 3, BX, BY * BZ), 1.0, 6.0, ((0, 8),), jnp.float32),
        "second_moment": jnp.clip(jnp.exp(math.log(4.0) - 2.0794415 * jax.random.uniform(streams_of[2], (BRICKS, 3, BX, BY * BZ), jnp.float32) ** shard_levels(streams_of[2], (BRICKS, 3, BX, BY * BZ), ((0, 8),), -0.2, 0.2)), 0.5, 4.0),
        "fiber": jnp.clip(jax.random.uniform(streams_of[3], (BRICKS, BX, BY * BZ), jnp.float32, -1.0, 1.0) * shard_levels(streams_of[3], (BRICKS, BX, BY * BZ), ((0, 8),), -0.4, 0.0), -1.0, 1.0),
        "measured": gaussian(streams_of[4], (FREQS, SUBZONES, 2, K * BX, BY * BZ), 1.0, 6.0, ((0, 4), (1, 8)), jnp.float32),
        "wave_sq": jnp.clip(jnp.exp(math.log(5.0) - 2.3025851 * jax.random.uniform(streams_of[5], (FREQS,), jnp.float32) ** shard_levels(streams_of[5], (FREQS,), ((0, 4),), -0.2, 0.2)), 0.5, 5.0),
        "send_list": draw_send_list(jax.random.fold_in(streams_of[8], 71), 0),
        "brick_list": draw_brick_list(jax.random.fold_in(streams_of[8], 71), 0),
    }


relax_rate = 0.25
learn_rate = 0.1
beta_first = 0.9
beta_second = 0.99
smooth_rate = 0.5
adam_eps = 1e-08

def beside_sum(cube):
    padded = jnp.pad(cube, ((0, 0), (1, 1), (1, 1), (1, 1)))
    total = padded[:, 2:, 1:-1, 1:-1] + padded[:, :-2, 1:-1, 1:-1]
    total = total + padded[:, 1:-1, 2:, 1:-1] + padded[:, 1:-1, :-2, 1:-1]
    return total + padded[:, 1:-1, 1:-1, 2:] + padded[:, 1:-1, 1:-1, :-2]

def misfit(moduli, fiber_tile, observed, wave_value):
    shear = (moduli[0] + (moduli[1] - moduli[0]) * fiber_tile * fiber_tile).reshape(-1, BY, BZ)
    damping = moduli[2].reshape(-1, BY, BZ)
    diagonal_term = 6.0 * shear + wave_value
    start_field = observed.reshape(2, -1, BY, BZ)
    field = start_field
    for sweep_index in range(SWEEPS):
        stencil = 6.0 * field - beside_sum(field)
        resid_real = shear * (stencil[0] - damping * stencil[1]) - wave_value * field[0]
        resid_imag = shear * (stencil[1] + damping * stencil[0]) - wave_value * field[1]
        field = field - relax_rate * jnp.stack([resid_real, resid_imag]) / diagonal_term
    gap = field - start_field
    return jnp.sum(gap * gap)

def update(moduli, first_moment, second_moment, fiber_tile, descent):
    new_first = beta_first * first_moment + (1.0 - beta_first) * descent
    new_second = beta_second * second_moment + (1.0 - beta_second) * descent * descent
    stepped = moduli - learn_rate * new_first / (jnp.sqrt(new_second) + adam_eps)
    shaped = stepped.reshape(stepped.shape[:-1] + (-1, BZ))
    lower_cell = jnp.concatenate([shaped[..., :1], shaped[..., :-1]], axis=-1).reshape(stepped.shape)
    upper_cell = jnp.concatenate([shaped[..., 1:], shaped[..., -1:]], axis=-1).reshape(stepped.shape)
    weight = smooth_rate * (fiber_tile * fiber_tile)[:, None]
    smoothed = stepped + weight * (0.5 * (lower_cell + upper_cell) - stepped)
    return (smoothed, new_first, new_second)

def reference(modulus, first_moment, second_moment, fiber, measured, wave_sq, send_list, brick_list):
    rows_brick = modulus.shape[2]
    depth = modulus.shape[3]
    owner_ids = (brick_list // CAP).astype(jnp.int32)
    slot_ids = (brick_list % CAP).astype(jnp.int32)
    dest_ids = (jnp.arange(SUBZONES, dtype=jnp.int32) // SZ_DEV)[:, None]
    local_ids = send_list[owner_ids, dest_ids, slot_ids]
    global_ids = (owner_ids * NB_DEV + local_ids).astype(jnp.int32)
    stacked = jnp.concatenate([modulus, fiber[:, None]], axis=1)

    def per_freq(grad_total, freq_item):
        observed_all, wave_value = freq_item

        def solve(subzone_item):
            brick_ids, observed = subzone_item
            picked_rows = stacked[brick_ids]
            subzone_par = jnp.swapaxes(picked_rows, 0, 1).reshape(4, K * rows_brick, depth)
            gradient = jax.grad(misfit)(subzone_par[:3], subzone_par[3], observed, wave_value)
            return jnp.swapaxes(gradient.reshape(3, K, rows_brick, depth), 0, 1)
        gradients = lax.map(solve, (global_ids, observed_all))
        grad_total = grad_total.at[global_ids.reshape(-1)].add(gradients.reshape(-1, 3, rows_brick, depth))
        return (grad_total, None)
    start_total = jnp.zeros((BRICKS, 3, rows_brick, depth), jnp.float32)
    grad_total, unused = lax.scan(per_freq, start_total, (measured, wave_sq))
    intersection = jnp.zeros((BRICKS,), jnp.float32).at[global_ids.reshape(-1)].add(1.0)
    descent = grad_total / (FREQS * jnp.maximum(intersection, 1.0))[:, None, None, None]
    return update(modulus, first_moment, second_moment, fiber, descent)
```

```python
import functools

import jax
import jax.numpy as jnp
from jax import lax
from jax.experimental import pallas as pl
from jax.experimental.pallas import tpu as pltpu
from jax.sharding import Mesh, PartitionSpec as P

BZ = 32
K = 8
SWEEPS = 6
LANES = 128
SUBL = 8

relax_rate = 0.25
learn_rate = 0.1
beta_first = 0.9
beta_second = 0.99
smooth_rate = 0.5
adam_eps = 1e-08

VMEM = pl.BlockSpec(memory_space=pltpu.VMEM)
SMEM = pl.BlockSpec(memory_space=pltpu.SMEM)


def pack_kernel(send_ref, brick_ref, modulus_ref, fiber_ref, out_ref, plane_ref):
    cap, zones = send_ref.shape
    owned = modulus_ref.shape[0]
    for b in range(owned):
        fib = fiber_ref[b]
        base = modulus_ref[b, 0]
        plane_ref[b, 0] = base + (modulus_ref[b, 1] - base) * fib * fib
        plane_ref[b, 1] = modulus_ref[b, 2]
    for d in range(zones):
        for c in range(cap):
            local = jnp.maximum(send_ref[c, d], 0)
            out_ref[d, c] = plane_ref[local]
    slot_at = lax.broadcasted_iota(jnp.int32, (SUBL, LANES), 1)
    for first in range(0, zones * cap, LANES):
        uses = jnp.zeros((SUBL, LANES), jnp.float32)
        for s in range(brick_ref.shape[0]):
            for k in range(brick_ref.shape[1]):
                uses = uses + jnp.where(slot_at == brick_ref[s, k] - first, 1.0, 0.0)
        for q in range(first, min(first + LANES, zones * cap)):
            wide = jnp.broadcast_to(uses[:, q - first : q - first + 1], (SUBL, LANES))
            out_ref[q // cap, cap + (q % cap) // 2, (q % cap) % 2] = wide


def solve_kernel(brick_ref, wave_ref, data_ref, seen_ref, out_ref, coef_ref, field_ref, sten_ref, lam_ref, grad_ref):
    subzones, entries = brick_ref.shape
    cap = out_ref.shape[2]
    wave = wave_ref[0]
    row = lax.broadcasted_iota(jnp.int32, (SUBL, LANES), 0)
    lane = lax.broadcasted_iota(jnp.int32, (SUBL, LANES), 1)
    z_first = lane % BZ == 0
    z_last = lane % BZ == BZ - 1
    low_lane = lane < BZ
    high_lane = lane >= LANES - BZ
    y_first = jnp.logical_and(row == 0, low_lane)
    y_last = jnp.logical_and(row == SUBL - 1, high_lane)

    def plane_sum(v):
        zm = jnp.where(z_first, 0.0, pltpu.roll(v, 1, 1))
        zp = jnp.where(z_last, 0.0, pltpu.roll(v, LANES - 1, 1))
        ym = pltpu.roll(v, BZ, 1)
        ym = jnp.where(low_lane, pltpu.roll(ym, 1, 0), ym)
        ym = jnp.where(y_first, 0.0, ym)
        yp = pltpu.roll(v, LANES - BZ, 1)
        yp = jnp.where(high_lane, pltpu.roll(yp, SUBL - 1, 0), yp)
        yp = jnp.where(y_last, 0.0, yp)
        return (zm + zp) + (ym + yp)

    def stencil(vs):
        sums = [plane_sum(v) for v in vs]
        res = []
        for x, v in enumerate(vs):
            total = sums[x]
            if x > 0:
                total = total + vs[x - 1]
            if x + 1 < len(vs):
                total = total + vs[x + 1]
            res.append(6.0 * v - total)
        return res

    for s in range(subzones):
        for k in range(entries):
            q = brick_ref[s, k]
            pair = data_ref[q // cap, q % cap]
            shear, damping = pair[0], pair[1]
            rate = relax_rate / (6.0 * shear + wave)
            beta = rate * shear
            coef_ref[s, 0, k] = 1.0 + rate * wave
            coef_ref[s, 1, k] = beta
            coef_ref[s, 2, k] = beta * damping
            for p in range(2):
                at = ((s * 2 + p) * SUBL) * K + k
                field_ref[0, s, p, k] = seen_ref[pl.ds(at, SUBL, stride=K), :]

    for t in range(SWEEPS):
        for s in range(subzones):
            old = [[field_ref[t, s, p, k] for k in range(entries)] for p in range(2)]
            sten = [stencil(old[p]) for p in range(2)]
            for k in range(entries):
                alpha, beta, gamma = coef_ref[s, 0, k], coef_ref[s, 1, k], coef_ref[s, 2, k]
                sr, si = sten[0][k], sten[1][k]
                sten_ref[t, s, 0, k] = sr
                sten_ref[t, s, 1, k] = si
                new_real = alpha * old[0][k] - (beta * sr - gamma * si)
                new_imag = alpha * old[1][k] - (beta * si + gamma * sr)
                if t + 1 < SWEEPS:
                    field_ref[t + 1, s, 0, k] = new_real
                    field_ref[t + 1, s, 1, k] = new_imag
                else:
                    lam_ref[s, 0, k] = new_real - field_ref[0, s, 0, k]
                    lam_ref[s, 1, k] = new_imag - field_ref[0, s, 1, k]

    for t in reversed(range(SWEEPS)):
        for s in range(subzones):
            back = [[], []]
            lams = [[lam_ref[s, p, k] for k in range(entries)] for p in range(2)]
            for k in range(entries):
                lr, li = lams[0][k], lams[1][k]
                fr, fi = field_ref[t, s, 0, k], field_ref[t, s, 1, k]
                sr, si = sten_ref[t, s, 0, k], sten_ref[t, s, 1, k]
                g_alpha = lr * fr + li * fi
                g_beta = lr * sr + li * si
                g_gamma = lr * si - li * sr
                if t + 1 < SWEEPS:
                    g_alpha = g_alpha + grad_ref[s, 0, k]
                    g_beta = g_beta + grad_ref[s, 1, k]
                    g_gamma = g_gamma + grad_ref[s, 2, k]
                grad_ref[s, 0, k] = g_alpha
                grad_ref[s, 1, k] = g_beta
                grad_ref[s, 2, k] = g_gamma
                if t > 0:
                    beta, gamma = coef_ref[s, 1, k], coef_ref[s, 2, k]
                    back[0].append(beta * lr + gamma * li)
                    back[1].append(beta * li - gamma * lr)
            if t > 0:
                for p in range(2):
                    sten = stencil(back[p])
                    for k in range(entries):
                        lam_ref[s, p, k] = coef_ref[s, 0, k] * lams[p][k] - sten[k]

    out_ref[...] = jnp.zeros_like(out_ref)
    for s in range(subzones):
        for k in range(entries):
            q = brick_ref[s, k]
            pair = data_ref[q // cap, q % cap]
            shear, damping = pair[0], pair[1]
            diag = 6.0 * shear + wave
            rate = relax_rate / diag
            g_alpha, g_beta, g_gamma = grad_ref[s, 0, k], grad_ref[s, 1, k], grad_ref[s, 2, k]
            mixed = damping * g_gamma - g_beta
            g_rate = wave * g_alpha + shear * mixed
            g_shear = rate * (mixed - 6.0 * g_rate / diag)
            g_damping = rate * shear * g_gamma
            for y in range(out_ref.shape[1]):
                out_ref[q // cap, y, q % cap, 0] += 2.0 * g_shear
                out_ref[q // cap, y, q % cap, 1] += 2.0 * g_damping


def update_kernel(
    freq_count, send_ref, mine_ref, other_ref, data_ref, modulus_ref, first_ref, second_ref, fiber_ref,
    modulus_out, first_out, second_out, total_ref, use_ref,
):
    cap, zones = send_ref.shape
    owned = modulus_ref.shape[0]
    lane = lax.broadcasted_iota(jnp.int32, (SUBL, LANES), 1)
    z_first = lane % BZ == 0
    z_last = lane % BZ == BZ - 1
    total_ref[...] = jnp.zeros_like(total_ref)
    use_ref[...] = jnp.zeros_like(use_ref)
    for d in range(zones):
        for c in range(cap):
            local = send_ref[c, d]
            local = jnp.where(local < 0, owned, local)
            got = total_ref[local]
            for y in range(mine_ref.shape[1]):
                got = got + (mine_ref[d, y, c] + other_ref[d, y, c])
            total_ref[local] = got
            use_ref[local] += data_ref[d, cap + c // 2, c % 2]
    for b in range(owned):
        fib = fiber_ref[b]
        fib_sq = fib * fib
        g_shear, g_damping = total_ref[b, 0], total_ref[b, 1]
        share = 1.0 / (freq_count * jnp.maximum(use_ref[b], 1.0))
        for p, grad in enumerate((g_shear * (1.0 - fib_sq), g_shear * fib_sq, g_damping)):
            descent = grad * share
            new_first = beta_first * first_ref[b, p] + (1.0 - beta_first) * descent
            new_second = beta_second * second_ref[b, p] + (1.0 - beta_second) * descent * descent
            stepped = modulus_ref[b, p] - learn_rate * new_first / (jnp.sqrt(new_second) + adam_eps)
            lower = jnp.where(z_first, stepped, pltpu.roll(stepped, 1, 1))
            upper = jnp.where(z_last, stepped, pltpu.roll(stepped, LANES - 1, 1))
            first_out[b, p] = new_first
            second_out[b, p] = new_second
            modulus_out[b, p] = stepped + smooth_rate * fib_sq * (0.5 * (lower + upper) - stepped)


def on_device(modulus, first_moment, second_moment, fiber, measured, wave_sq, send_list, brick_list):
    zones = lax.axis_size("zone")
    lines = lax.axis_size("line")
    cores = lax.axis_size("core")
    owned = modulus.shape[0]
    cells = (SUBL, LANES)
    cap = send_list.shape[2]
    subzones = brick_list.shape[0]
    send_table = send_list[0].T
    planes = lambda a: a.reshape(owned, 3, *cells)
    mod, first, second = planes(modulus), planes(first_moment), planes(second_moment)
    fib = fiber.reshape(owned, *cells)
    seen = measured.reshape(subzones, 2, K, SUBL, LANES).swapaxes(2, 3).reshape(-1, LANES)
    f32 = jnp.float32
    spare = (cap + 1) // 2
    outgoing = pl.pallas_call(
        pack_kernel,
        out_shape=jax.ShapeDtypeStruct((zones, cap + spare, 2, *cells), f32),
        in_specs=[SMEM, SMEM, VMEM, VMEM],
        out_specs=VMEM,
        scratch_shapes=[pltpu.VMEM((owned, 2, *cells), f32)],
        name="pack",
    )(send_table, brick_list, mod, fib)
    arrived = lax.all_to_all(outgoing, "zone", split_axis=0, concat_axis=0, tiled=True)
    state = (subzones, 2, K, *cells)
    slots = pl.pallas_call(
        solve_kernel,
        out_shape=jax.ShapeDtypeStruct((zones, lines, cap, 2, *cells), f32),
        in_specs=[SMEM, SMEM, VMEM, VMEM],
        out_specs=VMEM,
        scratch_shapes=[
            pltpu.VMEM((subzones, 3, K, *cells), f32),
            pltpu.VMEM((SWEEPS, *state), f32),
            pltpu.VMEM((SWEEPS, *state), f32),
            pltpu.VMEM(state, f32),
            pltpu.VMEM((subzones, 3, K, *cells), f32),
        ],
        name="solve",
    )(brick_list, wave_sq, arrived, seen)
    slots = slots.reshape(zones * lines, cap, 2, *cells)
    mine = lax.all_to_all(slots, ("zone", "line"), split_axis=0, concat_axis=0, tiled=True)
    if cores == 2:
        other = lax.ppermute(mine, "core", [(0, 1), (1, 0)])
    else:
        other = jnp.zeros_like(mine)
    mine, other = (a.reshape(zones, lines, cap, 2, *cells) for a in (mine, other))
    whole = jax.ShapeDtypeStruct((owned, 3, *cells), f32)
    results = pl.pallas_call(
        functools.partial(update_kernel, float(lines * cores)),
        out_shape=(whole, whole, whole),
        in_specs=[SMEM] + [VMEM] * 7,
        out_specs=(VMEM, VMEM, VMEM),
        scratch_shapes=[
            pltpu.VMEM((owned + 1, 2, *cells), f32),
            pltpu.VMEM((owned + 1, *cells), f32),
        ],
        name="update",
    )(send_table, mine, other, arrived, mod, first, second, fib)
    return tuple(r.reshape(modulus.shape) for r in results)


def solution(mesh):
    zones, freqs = mesh.shape["zone"], mesh.shape["freq"]
    cores = 2 if freqs % 2 == 0 else 1
    fine = Mesh(mesh.devices.reshape(zones, freqs // cores, cores), ("zone", "line", "core"))
    freq = ("line", "core")
    brick = P("zone", None, None, None)
    placed = (brick, brick, brick, P("zone", None, None), P(freq, "zone", None, None, None), P(freq), P("zone", None, None), P("zone", None))
    return jax.shard_map(on_device, mesh=fine, in_specs=placed, out_specs=(brick, brick, brick), check_vma=False)
```

```python
import functools

import jax
import jax.numpy as jnp
from jax import lax
from jax.experimental import pallas as pl
from jax.experimental.pallas import tpu as pltpu
from jax.sharding import Mesh, PartitionSpec as P

BZ = 32
K = 8
SWEEPS = 6
LANES = 128
SUBL = 8

relax_rate = 0.25
learn_rate = 0.1
beta_first = 0.9
beta_second = 0.99
smooth_rate = 0.5
adam_eps = 1e-08

VMEM = pl.BlockSpec(memory_space=pltpu.VMEM)
SMEM = pl.BlockSpec(memory_space=pltpu.SMEM)


def room(words):
    return pltpu.CompilerParams(vmem_limit_bytes=4 * words + 2**21)


def pack_kernel(send_ref, brick_ref, modulus_ref, fiber_ref, out_ref, plane_ref):
    cap, zones = send_ref.shape
    owned = modulus_ref.shape[0]
    for b in range(owned):
        fib = fiber_ref[b]
        base = modulus_ref[b, 0]
        plane_ref[b, 0] = base + (modulus_ref[b, 1] - base) * fib * fib
        plane_ref[b, 1] = modulus_ref[b, 2]
    for d in range(zones):
        for c in range(cap):
            local = jnp.maximum(send_ref[c, d], 0)
            out_ref[d, c] = plane_ref[local]
    slot_at = lax.broadcasted_iota(jnp.int32, (SUBL, LANES), 1)
    for first in range(0, zones * cap, LANES):
        uses = jnp.zeros((SUBL, LANES), jnp.float32)
        for s in range(brick_ref.shape[0]):
            for k in range(brick_ref.shape[1]):
                uses = uses + jnp.where(slot_at == brick_ref[s, k] - first, 1.0, 0.0)
        for q in range(first, min(first + LANES, zones * cap)):
            wide = jnp.broadcast_to(uses[:, q - first : q - first + 1], (SUBL, LANES))
            out_ref[q // cap, cap + (q % cap) // 2, (q % cap) % 2] = wide


def solve_kernel(brick_ref, wave_ref, data_ref, seen_ref, out_ref, coef_ref, field_ref, sten_ref, lam_ref, grad_ref):
    subzones, entries = brick_ref.shape
    cap = out_ref.shape[2]
    wave = wave_ref[0]
    row = lax.broadcasted_iota(jnp.int32, (SUBL, LANES), 0)
    lane = lax.broadcasted_iota(jnp.int32, (SUBL, LANES), 1)
    z_first = lane % BZ == 0
    z_last = lane % BZ == BZ - 1
    low_lane = lane < BZ
    high_lane = lane >= LANES - BZ
    y_first = jnp.logical_and(row == 0, low_lane)
    y_last = jnp.logical_and(row == SUBL - 1, high_lane)

    def plane_sum(v):
        zm = jnp.where(z_first, 0.0, pltpu.roll(v, 1, 1))
        zp = jnp.where(z_last, 0.0, pltpu.roll(v, LANES - 1, 1))
        ym = pltpu.roll(v, BZ, 1)
        ym = jnp.where(low_lane, pltpu.roll(ym, 1, 0), ym)
        ym = jnp.where(y_first, 0.0, ym)
        yp = pltpu.roll(v, LANES - BZ, 1)
        yp = jnp.where(high_lane, pltpu.roll(yp, SUBL - 1, 0), yp)
        yp = jnp.where(y_last, 0.0, yp)
        return (zm + zp) + (ym + yp)

    def stencil(vs):
        sums = [plane_sum(v) for v in vs]
        res = []
        for x, v in enumerate(vs):
            total = sums[x]
            if x > 0:
                total = total + vs[x - 1]
            if x + 1 < len(vs):
                total = total + vs[x + 1]
            res.append(6.0 * v - total)
        return res

    for s in range(subzones):
        for k in range(entries):
            q = brick_ref[s, k]
            pair = data_ref[q // cap, q % cap]
            shear, damping = pair[0], pair[1]
            rate = relax_rate / (6.0 * shear + wave)
            beta = rate * shear
            coef_ref[s, 0, k] = 1.0 + rate * wave
            coef_ref[s, 1, k] = beta
            coef_ref[s, 2, k] = beta * damping
            for p in range(2):
                at = ((s * 2 + p) * SUBL) * K + k
                field_ref[0, s, p, k] = seen_ref[pl.ds(at, SUBL, stride=K), :]

    for t in range(SWEEPS):
        for s in range(subzones):
            old = [[field_ref[t, s, p, k] for k in range(entries)] for p in range(2)]
            sten = [stencil(old[p]) for p in range(2)]
            for k in range(entries):
                alpha, beta, gamma = coef_ref[s, 0, k], coef_ref[s, 1, k], coef_ref[s, 2, k]
                sr, si = sten[0][k], sten[1][k]
                sten_ref[t, s, 0, k] = sr
                sten_ref[t, s, 1, k] = si
                new_real = alpha * old[0][k] - (beta * sr - gamma * si)
                new_imag = alpha * old[1][k] - (beta * si + gamma * sr)
                if t + 1 < SWEEPS:
                    field_ref[t + 1, s, 0, k] = new_real
                    field_ref[t + 1, s, 1, k] = new_imag
                else:
                    lam_ref[s, 0, k] = new_real - field_ref[0, s, 0, k]
                    lam_ref[s, 1, k] = new_imag - field_ref[0, s, 1, k]

    for t in reversed(range(SWEEPS)):
        for s in range(subzones):
            back = [[], []]
            lams = [[lam_ref[s, p, k] for k in range(entries)] for p in range(2)]
            for k in range(entries):
                lr, li = lams[0][k], lams[1][k]
                fr, fi = field_ref[t, s, 0, k], field_ref[t, s, 1, k]
                sr, si = sten_ref[t, s, 0, k], sten_ref[t, s, 1, k]
                g_alpha = lr * fr + li * fi
                g_beta = lr * sr + li * si
                g_gamma = lr * si - li * sr
                if t + 1 < SWEEPS:
                    g_alpha = g_alpha + grad_ref[s, 0, k]
                    g_beta = g_beta + grad_ref[s, 1, k]
                    g_gamma = g_gamma + grad_ref[s, 2, k]
                grad_ref[s, 0, k] = g_alpha
                grad_ref[s, 1, k] = g_beta
                grad_ref[s, 2, k] = g_gamma
                if t > 0:
                    beta, gamma = coef_ref[s, 1, k], coef_ref[s, 2, k]
                    back[0].append(beta * lr + gamma * li)
                    back[1].append(beta * li - gamma * lr)
            if t > 0:
                for p in range(2):
                    sten = stencil(back[p])
                    for k in range(entries):
                        lam_ref[s, p, k] = coef_ref[s, 0, k] * lams[p][k] - sten[k]

    out_ref[...] = jnp.zeros_like(out_ref)
    for s in range(subzones):
        for k in range(entries):
            q = brick_ref[s, k]
            pair = data_ref[q // cap, q % cap]
            shear, damping = pair[0], pair[1]
            diag = 6.0 * shear + wave
            rate = relax_rate / diag
            g_alpha, g_beta, g_gamma = grad_ref[s, 0, k], grad_ref[s, 1, k], grad_ref[s, 2, k]
            mixed = damping * g_gamma - g_beta
            g_rate = wave * g_alpha + shear * mixed
            g_shear = rate * (mixed - 6.0 * g_rate / diag)
            g_damping = rate * shear * g_gamma
            for y in range(out_ref.shape[1]):
                out_ref[q // cap, y, q % cap, 0] += 2.0 * g_shear
                out_ref[q // cap, y, q % cap, 1] += 2.0 * g_damping


def update_kernel(
    freq_count, send_ref, mine_ref, other_ref, data_ref, modulus_ref, first_ref, second_ref, fiber_ref,
    modulus_out, first_out, second_out, total_ref, use_ref,
):
    cap, zones = send_ref.shape
    owned = modulus_ref.shape[0]
    lane = lax.broadcasted_iota(jnp.int32, (SUBL, LANES), 1)
    z_first = lane % BZ == 0
    z_last = lane % BZ == BZ - 1
    total_ref[...] = jnp.zeros_like(total_ref)
    use_ref[...] = jnp.zeros_like(use_ref)
    for d in range(zones):
        for c in range(cap):
            local = send_ref[c, d]
            local = jnp.where(local < 0, owned, local)
            got = total_ref[local]
            for y in range(mine_ref.shape[1]):
                got = got + (mine_ref[d, y, c] + other_ref[d, y, c])
            total_ref[local] = got
            use_ref[local] += data_ref[d, cap + c // 2, c % 2]
    for b in range(owned):
        fib = fiber_ref[b]
        fib_sq = fib * fib
        g_shear, g_damping = total_ref[b, 0], total_ref[b, 1]
        share = 1.0 / (freq_count * jnp.maximum(use_ref[b], 1.0))
        for p, grad in enumerate((g_shear * (1.0 - fib_sq), g_shear * fib_sq, g_damping)):
            descent = grad * share
            new_first = beta_first * first_ref[b, p] + (1.0 - beta_first) * descent
            new_second = beta_second * second_ref[b, p] + (1.0 - beta_second) * descent * descent
            stepped = modulus_ref[b, p] - learn_rate * new_first / (jnp.sqrt(new_second) + adam_eps)
            lower = jnp.where(z_first, stepped, pltpu.roll(stepped, 1, 1))
            upper = jnp.where(z_last, stepped, pltpu.roll(stepped, LANES - 1, 1))
            first_out[b, p] = new_first
            second_out[b, p] = new_second
            modulus_out[b, p] = stepped + smooth_rate * fib_sq * (0.5 * (lower + upper) - stepped)


def on_device(modulus, first_moment, second_moment, fiber, measured, wave_sq, send_list, brick_list):
    zones = lax.axis_size("zone")
    lines = lax.axis_size("line")
    cores = lax.axis_size("core")
    owned = modulus.shape[0]
    cells = (SUBL, LANES)
    cap = send_list.shape[2]
    subzones = brick_list.shape[0]
    send_table = send_list[0].T
    planes = lambda a: a.reshape(owned, 3, *cells)
    mod, first, second = planes(modulus), planes(first_moment), planes(second_moment)
    fib = fiber.reshape(owned, *cells)
    seen = measured.reshape(subzones, 2, K, SUBL, LANES).swapaxes(2, 3).reshape(-1, LANES)
    f32 = jnp.float32
    spare = (cap + 1) // 2
    outgoing_size = zones * (cap + spare) * 2 * SUBL * LANES
    slot_size = zones * lines * cap * 2 * SUBL * LANES
    outgoing = pl.pallas_call(
        pack_kernel,
        out_shape=jax.ShapeDtypeStruct((zones, cap + spare, 2, *cells), f32),
        in_specs=[SMEM, SMEM, VMEM, VMEM],
        out_specs=VMEM,
        scratch_shapes=[pltpu.VMEM((owned, 2, *cells), f32)],
        name="pack",
    )(send_table, brick_list, mod, fib)
    arrived = lax.all_to_all(outgoing, "zone", split_axis=0, concat_axis=0, tiled=True)
    state = (subzones, 2, K, *cells)
    slots = pl.pallas_call(
        solve_kernel,
        out_shape=jax.ShapeDtypeStruct((zones, lines, cap, 2, *cells), f32),
        in_specs=[SMEM, SMEM, VMEM, VMEM],
        out_specs=VMEM,
        scratch_shapes=[
            pltpu.VMEM((subzones, 3, K, *cells), f32),
            pltpu.VMEM((SWEEPS, *state), f32),
            pltpu.VMEM((SWEEPS, *state), f32),
            pltpu.VMEM(state, f32),
            pltpu.VMEM((subzones, 3, K, *cells), f32),
        ],
        compiler_params=room(16 * SWEEPS * seen.size // 4 + 2 * outgoing_size + 2 * slot_size),
        name="solve",
    )(brick_list, wave_sq, arrived, seen)
    slots = slots.reshape(zones * lines, cap, 2, *cells)
    mine = lax.all_to_all(slots, ("zone", "line"), split_axis=0, concat_axis=0, tiled=True)
    if cores == 2:
        other = lax.ppermute(mine, "core", [(0, 1), (1, 0)])
    else:
        other = jnp.zeros_like(mine)
    mine, other = (a.reshape(zones, lines, cap, 2, *cells) for a in (mine, other))
    whole = jax.ShapeDtypeStruct((owned, 3, *cells), f32)
    results = pl.pallas_call(
        functools.partial(update_kernel, float(lines * cores)),
        out_shape=(whole, whole, whole),
        in_specs=[SMEM] + [VMEM] * 7,
        out_specs=(VMEM, VMEM, VMEM),
        scratch_shapes=[
            pltpu.VMEM((owned + 1, 2, *cells), f32),
            pltpu.VMEM((owned + 1, *cells), f32),
        ],
        compiler_params=room(10 * modulus.size + outgoing_size + 2 * slot_size),
        name="update",
    )(send_table, mine, other, arrived, mod, first, second, fib)
    return tuple(r.reshape(modulus.shape) for r in results)


def solution(mesh):
    zones, freqs = mesh.shape["zone"], mesh.shape["freq"]
    cores = 2 if freqs % 2 == 0 else 1
    fine = Mesh(mesh.devices.reshape(zones, freqs // cores, cores), ("zone", "line", "core"))
    freq = ("line", "core")
    brick = P("zone", None, None, None)
    placed = (brick, brick, brick, P("zone", None, None), P(freq, "zone", None, None, None), P(freq), P("zone", None, None), P("zone", None))
    return jax.shard_map(on_device, mesh=fine, in_specs=placed, out_specs=(brick, brick, brick), check_vma=False)
```

```python
import functools

import jax
import jax.numpy as jnp
from jax import lax
from jax.experimental import pallas as pl
from jax.experimental.pallas import tpu as pltpu
from jax.sharding import Mesh, PartitionSpec as P

BZ = 32
K = 8
SWEEPS = 6
LANES = 128
SUBL = 8

relax_rate = 0.25
learn_rate = 0.1
beta_first = 0.9
beta_second = 0.99
smooth_rate = 0.5
adam_eps = 1e-08

VMEM = pl.BlockSpec(memory_space=pltpu.VMEM)
SMEM = pl.BlockSpec(memory_space=pltpu.SMEM)
HBM = pl.BlockSpec(memory_space=pltpu.HBM)


def room(words):
    return pltpu.CompilerParams(vmem_limit_bytes=4 * words + 2**21)


def pack_kernel(
    send_hbm, brick_hbm, modulus_hbm, fiber_hbm,
    out_ref, send_out, brick_out,
    send_ref, brick_ref, modulus_ref, fiber_ref, plane_ref, sems,
):
    pairs = (
        (send_hbm, send_ref), (brick_hbm, brick_ref), (modulus_hbm, modulus_ref), (fiber_hbm, fiber_ref),
        (send_hbm, send_out), (brick_hbm, brick_out),
    )
    copies = [pltpu.make_async_copy(a, b, sems.at[i]) for i, (a, b) in enumerate(pairs)]
    for copy in copies:
        copy.start()
    for copy in copies[:4]:
        copy.wait()
    cap, zones = send_ref.shape
    owned = modulus_ref.shape[0]
    for b in range(owned):
        fib = fiber_ref[b]
        base = modulus_ref[b, 0]
        plane_ref[b, 0] = base + (modulus_ref[b, 1] - base) * fib * fib
        plane_ref[b, 1] = modulus_ref[b, 2]
    slot_at = lax.broadcasted_iota(jnp.int32, (SUBL, LANES), 1)
    for first in range(0, zones * cap, LANES):
        uses = jnp.zeros((SUBL, LANES), jnp.float32)
        for s in range(brick_ref.shape[0]):
            for k in range(brick_ref.shape[1]):
                uses = uses + jnp.where(slot_at == brick_ref[s, k] - first, 1.0, 0.0)
        for q in range(first, min(first + LANES, zones * cap)):
            wide = jnp.broadcast_to(uses[:1, q - first : q - first + 1], (1, LANES))
            row = 2 * SUBL * cap + q % cap
            out_ref[q // cap, row : row + 1] = wide
    for d in range(zones):
        for c in range(cap):
            local = jnp.maximum(send_ref[c, d], 0)
            for p in range(2):
                row = (2 * c + p) * SUBL
                out_ref[d, row : row + SUBL] = plane_ref[local, p]
        row = 2 * SUBL * cap + cap
        if row < out_ref.shape[1]:
            out_ref[d, row:] = jnp.zeros((out_ref.shape[1] - row, LANES), jnp.float32)
    for copy in copies[4:]:
        copy.wait()


def stencil(v, table_ref, res_ref):
    rows = v[0][0].shape[0]
    flat = jnp.concatenate([tile for line in v for tile in line], axis=0)
    high = flat.astype(jnp.bfloat16)
    low = (flat - high.astype(jnp.float32)).astype(jnp.bfloat16)
    res_ref[...] = jnp.dot(
        jnp.concatenate([high, low], axis=1), table_ref[...], preferred_element_type=jnp.float32
    )
    lane = lax.broadcasted_iota(jnp.int32, (rows, LANES), 1)
    low_half = lane < LANES // 2
    res = []
    for x, line in enumerate(v):
        res.append([])
        for y in range(len(line)):
            at = (x * len(line) + y) * rows
            below = res_ref[at - rows : at, LANES:] if y > 0 else 0.0
            above = res_ref[at + rows : at + 2 * rows, LANES:] if y + 1 < len(line) else 0.0
            total = res_ref[at : at + rows, :LANES] + jnp.where(low_half, below, above)
            sides = [v[i][y] for i in (x - 1, x + 1) if 0 <= i < len(v)]
            res[-1].append(total - sum(sides[1:], sides[0]))
    return res


def prepare_kernel(seen_ref, field_out, sten_out, table_out, res_ref):
    source = lax.broadcasted_iota(jnp.int32, table_out.shape, 0) % LANES
    column = lax.broadcasted_iota(jnp.int32, table_out.shape, 1)
    target = column % LANES
    step = jnp.abs(source - target)
    beside = jnp.logical_or(step == BZ, jnp.logical_and(step == 1, source // BZ == target // BZ))
    inner = jnp.where(step == 0, 6.0, jnp.where(beside, -1.0, 0.0))
    wrap = jnp.where(step == LANES - BZ, -1.0, 0.0)
    table_out[...] = jnp.where(column < LANES, inner, wrap).astype(table_out.dtype)
    lines, subl, rows, _ = field_out.shape
    subzones = rows // 2
    for x in range(lines):
        for y in range(subl):
            for p in range(2):
                at = p * subl * lines + y * lines + x
                field_out[x, y, p * subzones : (p + 1) * subzones] = seen_ref[
                    pl.ds(at, subzones, stride=2 * subl * lines), :
                ]
    sten = stencil([[field_out[x, y] for y in range(subl)] for x in range(lines)], table_out, res_ref)
    for x in range(lines):
        for y in range(subl):
            sten_out[x, y] = sten[x][y]


def solve_kernel(
    brick_ref, wave_ref, data_ref, start_ref, sten0_ref, table_ref, out_ref,
    coef_ref, field_ref, sten_ref, lam_ref, grad_ref, res_ref, sum_ref,
):
    subzones, entries = brick_ref.shape
    rows = 2 * subzones
    cap = out_ref.shape[2]
    slots = out_ref.shape[0] * cap
    wave = wave_ref[0]
    grid = [(x, y) for x in range(entries) for y in range(SUBL)]

    def swap(v):
        return pltpu.roll(v, subzones, 0)

    def moduli(s, k):
        q = brick_ref[s, k]
        shear = data_ref[q // cap, pl.ds(pl.multiple_of(q % cap * 2 * SUBL, SUBL), SUBL)]
        damping = data_ref[q // cap, pl.ds(pl.multiple_of((q % cap * 2 + 1) * SUBL, SUBL), SUBL)]
        return shear, damping

    def rows_of(p, s, k):
        return pl.ds(k * SUBL * rows + p * subzones + s, SUBL, stride=rows)

    for s in range(subzones):
        for k in range(entries):
            shear, damping = moduli(s, k)
            rate = relax_rate / (6.0 * shear + wave)
            alpha = 1.0 + rate * wave
            beta = rate * shear
            gamma = beta * damping
            for p in range(2):
                coef_ref[0, rows_of(p, s, k), :] = alpha
                coef_ref[1, rows_of(p, s, k), :] = beta
                coef_ref[2, rows_of(p, s, k), :] = gamma if p == 0 else -gamma

    def coef(i, x, y):
        at = (x * SUBL + y) * rows
        return coef_ref[i, at : at + rows]

    def field(t, x, y):
        return field_ref[t - 1, x, y] if t > 0 else start_ref[x, y]

    for t in range(SWEEPS):
        if t == 0:
            sten = [[sten0_ref[x, y] for y in range(SUBL)] for x in range(entries)]
        else:
            sten = stencil([[field(t, x, y) for y in range(SUBL)] for x in range(entries)], table_ref, res_ref)
        for x, y in grid:
            own = sten[x][y]
            turned = swap(own)
            sten_ref[t, 0, x, y] = own
            sten_ref[t, 1, x, y] = turned
            new = coef(0, x, y) * field(t, x, y) - coef(1, x, y) * own + coef(2, x, y) * turned
            if t + 1 < SWEEPS:
                field_ref[t, x, y] = new
            else:
                lam_ref[x, y] = new - start_ref[x, y]

    for t in reversed(range(SWEEPS)):
        back = [[None] * SUBL for _ in range(entries)]
        for x, y in grid:
            lam = lam_ref[x, y]
            parts = (lam * field(t, x, y), lam * sten_ref[t, 0, x, y], lam * sten_ref[t, 1, x, y])
            at = (x * SUBL + y) * rows
            for i, part in enumerate(parts):
                if t + 1 < SWEEPS:
                    part = part + grad_ref[i, at : at + rows]
                grad_ref[i, at : at + rows] = part
            if t > 0:
                back[x][y] = coef(1, x, y) * lam + coef(2, x, y) * swap(lam)
        if t > 0:
            sten = stencil(back, table_ref, res_ref)
            for x, y in grid:
                lam_ref[x, y] = coef(0, x, y) * lam_ref[x, y] - sten[x][y]

    sum_ref[...] = jnp.zeros_like(sum_ref)
    for s in range(subzones):
        for k in range(entries):
            shear, damping = moduli(s, k)
            diag = 6.0 * shear + wave
            rate = relax_rate / diag
            real, imag = ([grad_ref[i, rows_of(p, s, k), :] for i in range(3)] for p in range(2))
            g_alpha, g_beta, g_gamma = real[0] + imag[0], real[1] + imag[1], real[2] - imag[2]
            mixed = damping * g_gamma - g_beta
            g_rate = wave * g_alpha + shear * mixed
            q = brick_ref[s, k]
            sum_ref[s, q, 0] += rate * (mixed - 6.0 * g_rate / diag)
            sum_ref[s, q, 1] += rate * shear * g_gamma
    for q in range(slots):
        for p in range(2):
            total = sum_ref[0, q, p]
            for s in range(1, subzones):
                total = total + sum_ref[s, q, p]
            total = 2.0 * total
            for y in range(out_ref.shape[1]):
                out_ref[q // cap, y, q % cap, p] = total


def update_kernel(
    freq_count, send_ref, mine_ref, other_ref, data_ref, modulus_ref, first_ref, second_ref, fiber_ref,
    modulus_out, first_out, second_out, total_ref, use_ref,
):
    cap, zones = send_ref.shape
    owned = modulus_ref.shape[0]
    lane = lax.broadcasted_iota(jnp.int32, (SUBL, LANES), 1)
    z_first = lane % BZ == 0
    z_last = lane % BZ == BZ - 1
    total_ref[...] = jnp.zeros_like(total_ref)
    use_ref[...] = jnp.zeros_like(use_ref)
    for d in range(zones):
        for c in range(cap):
            local = send_ref[c, d]
            local = jnp.where(local < 0, owned, local)
            got = total_ref[local]
            for y in range(mine_ref.shape[1]):
                got = got + (mine_ref[d, y, c] + other_ref[d, y, c])
            total_ref[local] = got
            use_ref[local] += data_ref[d, pl.ds(2 * SUBL * cap + c, 1)]
    for b in range(owned):
        fib = fiber_ref[b]
        fib_sq = fib * fib
        g_shear, g_damping = total_ref[b, 0], total_ref[b, 1]
        share = 1.0 / (freq_count * jnp.maximum(use_ref[b], 1.0))
        for p, grad in enumerate((g_shear * (1.0 - fib_sq), g_shear * fib_sq, g_damping)):
            descent = grad * share
            new_first = beta_first * first_ref[b, p] + (1.0 - beta_first) * descent
            new_second = beta_second * second_ref[b, p] + (1.0 - beta_second) * descent * descent
            stepped = modulus_ref[b, p] - learn_rate * new_first / (jnp.sqrt(new_second) + adam_eps)
            lower = jnp.where(z_first, stepped, pltpu.roll(stepped, 1, 1))
            upper = jnp.where(z_last, stepped, pltpu.roll(stepped, LANES - 1, 1))
            first_out[b, p] = new_first
            second_out[b, p] = new_second
            modulus_out[b, p] = stepped + smooth_rate * fib_sq * (0.5 * (lower + upper) - stepped)


def on_device(modulus, first_moment, second_moment, fiber, measured, wave_sq, send_list, brick_list):
    zones = lax.axis_size("zone")
    lines = lax.axis_size("line")
    cores = lax.axis_size("core")
    owned = modulus.shape[0]
    cells = (SUBL, LANES)
    cap = send_list.shape[2]
    subzones = brick_list.shape[0]
    planes = lambda a: a.reshape(owned, 3, *cells)
    mod, first, second = planes(modulus), planes(first_moment), planes(second_moment)
    fib = fiber.reshape(owned, *cells)
    seen = measured.reshape(subzones, 2, K, SUBL, LANES).swapaxes(2, 3).reshape(-1, LANES)
    f32 = jnp.float32
    rows = 2 * SUBL * cap + -(-cap // SUBL) * SUBL
    outgoing_size = zones * rows * LANES
    slot_size = zones * lines * cap * 2 * SUBL * LANES
    i32 = jnp.int32
    shape = jax.ShapeDtypeStruct
    outgoing, send_table, bricks = pl.pallas_call(
        pack_kernel,
        out_shape=(
            shape((zones, rows, LANES), f32), shape((cap, zones), i32), shape(brick_list.shape, i32),
        ),
        in_specs=[HBM] * 4,
        out_specs=(VMEM,) * 3,
        scratch_shapes=[
            pltpu.SMEM((cap, zones), i32),
            pltpu.SMEM(brick_list.shape, i32),
            pltpu.VMEM((owned, 3, *cells), f32),
            pltpu.VMEM((owned, *cells), f32),
            pltpu.VMEM((owned, 2, *cells), f32),
            pltpu.SemaphoreType.DMA((6,)),
        ],
        compiler_params=room(outgoing_size + 4 * modulus.size),
        name="pack",
    )(*(pltpu.with_memory_space_constraint(a, pltpu.HBM) for a in (send_list[0].T, brick_list, mod, fib)))
    arrived = lax.all_to_all(outgoing, "zone", split_axis=0, concat_axis=0, tiled=True)
    state = (K, SUBL, 2 * subzones, LANES)
    sites = K * SUBL * 2 * subzones
    table = (2 * LANES, 2 * LANES)
    start, sten0, neighbours = pl.pallas_call(
        prepare_kernel,
        out_shape=(shape(state, f32), shape(state, f32), shape(table, jnp.bfloat16)),
        in_specs=[VMEM],
        out_specs=(VMEM,) * 3,
        scratch_shapes=[pltpu.VMEM((sites, 2 * LANES), f32)],
        compiler_params=room(8 * seen.size),
        cost_estimate=pl.CostEstimate(flops=2**24, bytes_accessed=16 * seen.size, transcendentals=0),
        name="prepare",
    )(seen)
    slots = pl.pallas_call(
        solve_kernel,
        out_shape=shape((zones, lines, cap, 2, *cells), f32),
        in_specs=[SMEM, SMEM] + [VMEM] * 4,
        out_specs=VMEM,
        scratch_shapes=[
            pltpu.VMEM((3, sites, LANES), f32),
            pltpu.VMEM((SWEEPS - 1, *state), f32),
            pltpu.VMEM((SWEEPS, 2, *state), f32),
            pltpu.VMEM(state, f32),
            pltpu.VMEM((3, sites, LANES), f32),
            pltpu.VMEM((sites, 2 * LANES), f32),
            pltpu.VMEM((subzones, zones * cap, 2, *cells), f32),
        ],
        compiler_params=room((8 * SWEEPS + 8) * seen.size + 2 * outgoing_size + (2 + subzones) * slot_size),
        name="solve",
    )(bricks, wave_sq, arrived, start, sten0, neighbours)
    slots = slots.reshape(zones * lines, cap, 2, *cells)
    mine = lax.all_to_all(slots, ("zone", "line"), split_axis=0, concat_axis=0, tiled=True)
    if cores == 2:
        other = lax.ppermute(mine, "core", [(0, 1), (1, 0)])
    else:
        other = jnp.zeros_like(mine)
    mine, other = (a.reshape(zones, lines, cap, 2, *cells) for a in (mine, other))
    whole = jax.ShapeDtypeStruct((owned, 3, *cells), f32)
    results = pl.pallas_call(
        functools.partial(update_kernel, float(lines * cores)),
        out_shape=(whole, whole, whole),
        in_specs=[SMEM] + [VMEM] * 7,
        out_specs=(VMEM, VMEM, VMEM),
        scratch_shapes=[
            pltpu.VMEM((owned + 1, 2, *cells), f32),
            pltpu.VMEM((owned + 1, 1, LANES), f32),
        ],
        compiler_params=room(10 * modulus.size + outgoing_size + 2 * slot_size),
        name="update",
    )(send_table, mine, other, arrived, mod, first, second, fib)
    return tuple(r.reshape(modulus.shape) for r in results)


def solution(mesh):
    zones, freqs = mesh.shape["zone"], mesh.shape["freq"]
    cores = 2 if freqs % 2 == 0 else 1
    fine = Mesh(mesh.devices.reshape(zones, freqs // cores, cores), ("zone", "line", "core"))
    freq = ("line", "core")
    brick = P("zone", None, None, None)
    placed = (brick, brick, brick, P("zone", None, None), P(freq, "zone", None, None, None), P(freq), P("zone", None, None), P("zone", None))
    return jax.shard_map(on_device, mesh=fine, in_specs=placed, out_specs=(brick, brick, brick), check_vma=False)
```

```python
import functools

import jax
import jax.numpy as jnp
from jax import lax
from jax.experimental import pallas as pl
from jax.experimental.pallas import tpu as pltpu
from jax.sharding import Mesh, PartitionSpec as P

BZ = 32
K = 8
SWEEPS = 6
LANES = 128
SUBL = 8

relax_rate = 0.25
learn_rate = 0.1
beta_first = 0.9
beta_second = 0.99
smooth_rate = 0.5
adam_eps = 1e-08

VMEM = pl.BlockSpec(memory_space=pltpu.VMEM)
SMEM = pl.BlockSpec(memory_space=pltpu.SMEM)
HBM = pl.BlockSpec(memory_space=pltpu.HBM)


def room(words):
    return pltpu.CompilerParams(vmem_limit_bytes=4 * words + 2**21)


def pack_kernel(
    send_hbm, brick_hbm, modulus_hbm, fiber_hbm,
    out_ref, send_out, brick_out,
    send_ref, brick_ref, slot_ref, modulus_ref, fiber_ref, plane_ref, sems,
):
    pairs = (
        (send_hbm, send_ref), (brick_hbm, brick_ref), (modulus_hbm, modulus_ref), (fiber_hbm, fiber_ref),
        (send_hbm, send_out), (brick_hbm, slot_ref),
    )
    copies = [pltpu.make_async_copy(a, b, sems.at[i]) for i, (a, b) in enumerate(pairs)]
    for copy in copies:
        copy.start()
    for copy in copies[:4]:
        copy.wait()
    cap, zones = send_ref.shape
    owned = modulus_ref.shape[0]
    for b in range(owned):
        fib = fiber_ref[b]
        base = modulus_ref[b, 0]
        plane_ref[b, 0] = base + (modulus_ref[b, 1] - base) * fib * fib
        plane_ref[b, 1] = modulus_ref[b, 2]
    slot_at = lax.broadcasted_iota(jnp.int32, (SUBL, LANES), 1)
    for first in range(0, zones * cap, LANES):
        uses = jnp.zeros((SUBL, LANES), jnp.float32)
        for s in range(brick_ref.shape[0]):
            for k in range(brick_ref.shape[1]):
                uses = uses + jnp.where(slot_at == brick_ref[s, k] - first, 1.0, 0.0)
        for q in range(first, min(first + LANES, zones * cap)):
            wide = jnp.broadcast_to(uses[:1, q - first : q - first + 1], (1, LANES))
            row = 2 * SUBL * cap + q % cap
            out_ref[q // cap, row : row + 1] = wide
    for d in range(zones):
        for c in range(cap):
            local = jnp.maximum(send_ref[c, d], 0)
            for p in range(2):
                row = (2 * c + p) * SUBL
                out_ref[d, row : row + SUBL] = plane_ref[local, p]
        row = 2 * SUBL * cap + cap
        if row < out_ref.shape[1]:
            out_ref[d, row:] = jnp.zeros((out_ref.shape[1] - row, LANES), jnp.float32)
    for copy in copies[4:]:
        copy.wait()
    slot = slot_ref[...]
    owner = jnp.zeros_like(slot)
    for d in range(1, zones):
        owner = owner + jnp.where(slot >= d * cap, 1, 0)
    brick_out[...] = owner * out_ref.shape[1] + (slot - owner * cap) * (2 * SUBL)


def stencil(v, table_ref, res_ref):
    rows = v[0][0].shape[0]
    flat = jnp.concatenate([tile for line in v for tile in line], axis=0)
    high = flat.astype(jnp.bfloat16)
    low = (flat - high.astype(jnp.float32)).astype(jnp.bfloat16)
    res_ref[...] = jnp.dot(
        jnp.concatenate([high, low], axis=1), table_ref[...], preferred_element_type=jnp.float32
    )
    lane = lax.broadcasted_iota(jnp.int32, (rows, LANES), 1)
    low_half = lane < LANES // 2
    res = []
    for x, line in enumerate(v):
        res.append([])
        for y in range(len(line)):
            at = (x * len(line) + y) * rows
            below = res_ref[at - rows : at, LANES:] if y > 0 else 0.0
            above = res_ref[at + rows : at + 2 * rows, LANES:] if y + 1 < len(line) else 0.0
            total = res_ref[at : at + rows, :LANES] + jnp.where(low_half, below, above)
            sides = [v[i][y] for i in (x - 1, x + 1) if 0 <= i < len(v)]
            res[-1].append(total - sum(sides[1:], sides[0]))
    return res


def prepare_kernel(seen_ref, field_out, sten_out, table_out, res_ref):
    source = lax.broadcasted_iota(jnp.int32, table_out.shape, 0) % LANES
    column = lax.broadcasted_iota(jnp.int32, table_out.shape, 1)
    target = column % LANES
    step = jnp.abs(source - target)
    beside = jnp.logical_or(step == BZ, jnp.logical_and(step == 1, source // BZ == target // BZ))
    inner = jnp.where(step == 0, 6.0, jnp.where(beside, -1.0, 0.0))
    wrap = jnp.where(step == LANES - BZ, -1.0, 0.0)
    table_out[...] = jnp.where(column < LANES, inner, wrap).astype(table_out.dtype)
    lines, subl, rows, _ = field_out.shape
    subzones = rows // 2
    for x in range(lines):
        for y in range(subl):
            for p in range(2):
                at = p * subl * lines + y * lines + x
                field_out[x, y, p * subzones : (p + 1) * subzones] = seen_ref[
                    pl.ds(at, subzones, stride=2 * subl * lines), :
                ]
    sten = stencil([[field_out[x, y] for y in range(subl)] for x in range(lines)], table_out, res_ref)
    for x in range(lines):
        for y in range(subl):
            sten_out[x, y] = sten[x][y]


def solve_kernel(
    brick_ref, wave_ref, data_ref, start_ref, sten0_ref, table_ref, out_ref,
    coef_ref, field_ref, sten_ref, lam_ref, grad_ref, res_ref, sum_ref,
):
    subzones, entries = brick_ref.shape
    rows = 2 * subzones
    cap = out_ref.shape[2]
    pitch = data_ref.shape[0] // out_ref.shape[0]
    wave = wave_ref[0]
    table = brick_ref[...]
    starts = [[pl.multiple_of(table[s, k], SUBL) for k in range(entries)] for s in range(subzones)]
    grid = [(x, y) for x in range(entries) for y in range(SUBL)]

    def swap(v):
        return pltpu.roll(v, subzones, 0)

    def moduli(s, k):
        return data_ref[pl.ds(starts[s][k], SUBL)], data_ref[pl.ds(starts[s][k] + SUBL, SUBL)]

    def rows_of(p, s, k):
        return pl.ds(k * SUBL * rows + p * subzones + s, SUBL, stride=rows)

    for s in range(subzones):
        for k in range(entries):
            shear, damping = moduli(s, k)
            rate = relax_rate / (6.0 * shear + wave)
            alpha = 1.0 + rate * wave
            beta = rate * shear
            gamma = beta * damping
            for p in range(2):
                coef_ref[0, rows_of(p, s, k), :] = alpha
                coef_ref[1, rows_of(p, s, k), :] = beta
                coef_ref[2, rows_of(p, s, k), :] = gamma if p == 0 else -gamma

    def coef(i, x, y):
        at = (x * SUBL + y) * rows
        return coef_ref[i, at : at + rows]

    def field(t, x, y):
        return field_ref[t - 1, x, y] if t > 0 else start_ref[x, y]

    for t in range(SWEEPS):
        if t == 0:
            sten = [[sten0_ref[x, y] for y in range(SUBL)] for x in range(entries)]
        else:
            sten = stencil([[field(t, x, y) for y in range(SUBL)] for x in range(entries)], table_ref, res_ref)
        for x, y in grid:
            own = sten[x][y]
            turned = swap(own)
            sten_ref[t, 0, x, y] = own
            sten_ref[t, 1, x, y] = turned
            new = coef(0, x, y) * field(t, x, y) - coef(1, x, y) * own + coef(2, x, y) * turned
            if t + 1 < SWEEPS:
                field_ref[t, x, y] = new
            else:
                lam_ref[x, y] = new - start_ref[x, y]

    for t in reversed(range(SWEEPS)):
        back = [[None] * SUBL for _ in range(entries)]
        for x, y in grid:
            lam = lam_ref[x, y]
            parts = (lam * field(t, x, y), lam * sten_ref[t, 0, x, y], lam * sten_ref[t, 1, x, y])
            at = (x * SUBL + y) * rows
            for i, part in enumerate(parts):
                if t + 1 < SWEEPS:
                    part = part + grad_ref[i, at : at + rows]
                grad_ref[i, at : at + rows] = part
            if t > 0:
                back[x][y] = coef(1, x, y) * lam + coef(2, x, y) * swap(lam)
        if t > 0:
            sten = stencil(back, table_ref, res_ref)
            for x, y in grid:
                lam_ref[x, y] = coef(0, x, y) * lam_ref[x, y] - sten[x][y]

    sum_ref[...] = jnp.zeros_like(sum_ref)
    for s in range(subzones):
        for k in range(entries):
            shear, damping = moduli(s, k)
            diag = 6.0 * shear + wave
            rate = relax_rate / diag
            real, imag = ([grad_ref[i, rows_of(p, s, k), :] for i in range(3)] for p in range(2))
            g_alpha, g_beta, g_gamma = real[0] + imag[0], real[1] + imag[1], real[2] - imag[2]
            mixed = damping * g_gamma - g_beta
            g_rate = wave * g_alpha + shear * mixed
            sum_ref[s, pl.ds(starts[s][k], SUBL)] += rate * (mixed - 6.0 * g_rate / diag)
            sum_ref[s, pl.ds(starts[s][k] + SUBL, SUBL)] += rate * shear * g_gamma
    for o in range(out_ref.shape[0]):
        for c in range(cap):
            for p in range(2):
                at = o * pitch + (2 * c + p) * SUBL
                total = sum_ref[0, at : at + SUBL]
                for s in range(1, subzones):
                    total = total + sum_ref[s, at : at + SUBL]
                total = 2.0 * total
                for y in range(out_ref.shape[1]):
                    out_ref[o, y, c, p] = total


def update_kernel(
    freq_count, send_ref, mine_ref, other_ref, data_ref, modulus_ref, first_ref, second_ref, fiber_ref,
    modulus_out, first_out, second_out, total_ref, use_ref,
):
    cap, zones = send_ref.shape
    owned = modulus_ref.shape[0]
    lane = lax.broadcasted_iota(jnp.int32, (SUBL, LANES), 1)
    z_first = lane % BZ == 0
    z_last = lane % BZ == BZ - 1
    table = send_ref[...]
    total_ref[...] = jnp.zeros_like(total_ref)
    use_ref[...] = jnp.zeros_like(use_ref)
    for d in range(zones):
        for c in range(cap):
            local = table[c, d]
            local = jnp.where(local < 0, owned, local)
            got = total_ref[local]
            for y in range(mine_ref.shape[1]):
                got = got + (mine_ref[d, y, c] + other_ref[d, y, c])
            total_ref[local] = got
            use_ref[local] += data_ref[d, pl.ds(2 * SUBL * cap + c, 1)]
    for b in range(owned):
        fib = fiber_ref[b]
        fib_sq = fib * fib
        g_shear, g_damping = total_ref[b, 0], total_ref[b, 1]
        share = 1.0 / (freq_count * jnp.maximum(use_ref[b], 1.0))
        for p, grad in enumerate((g_shear * (1.0 - fib_sq), g_shear * fib_sq, g_damping)):
            descent = grad * share
            new_first = beta_first * first_ref[b, p] + (1.0 - beta_first) * descent
            new_second = beta_second * second_ref[b, p] + (1.0 - beta_second) * descent * descent
            stepped = modulus_ref[b, p] - learn_rate * new_first / (jnp.sqrt(new_second) + adam_eps)
            lower = jnp.where(z_first, stepped, pltpu.roll(stepped, 1, 1))
            upper = jnp.where(z_last, stepped, pltpu.roll(stepped, LANES - 1, 1))
            first_out[b, p] = new_first
            second_out[b, p] = new_second
            modulus_out[b, p] = stepped + smooth_rate * fib_sq * (0.5 * (lower + upper) - stepped)


def on_device(modulus, first_moment, second_moment, fiber, measured, wave_sq, send_list, brick_list):
    zones = lax.axis_size("zone")
    lines = lax.axis_size("line")
    cores = lax.axis_size("core")
    owned = modulus.shape[0]
    cells = (SUBL, LANES)
    cap = send_list.shape[2]
    subzones = brick_list.shape[0]
    planes = lambda a: a.reshape(owned, 3, *cells)
    mod, first, second = planes(modulus), planes(first_moment), planes(second_moment)
    fib = fiber.reshape(owned, *cells)
    seen = measured.reshape(subzones, 2, K, SUBL, LANES).swapaxes(2, 3).reshape(-1, LANES)
    f32 = jnp.float32
    rows = 2 * SUBL * cap + -(-cap // SUBL) * SUBL
    outgoing_size = zones * rows * LANES
    slot_size = zones * lines * cap * 2 * SUBL * LANES
    i32 = jnp.int32
    shape = jax.ShapeDtypeStruct
    outgoing, send_table, bricks = pl.pallas_call(
        pack_kernel,
        out_shape=(
            shape((zones, rows, LANES), f32), shape((cap, zones), i32), shape(brick_list.shape, i32),
        ),
        in_specs=[HBM] * 4,
        out_specs=(VMEM,) * 3,
        scratch_shapes=[
            pltpu.SMEM((cap, zones), i32),
            pltpu.SMEM(brick_list.shape, i32),
            pltpu.VMEM(brick_list.shape, i32),
            pltpu.VMEM((owned, 3, *cells), f32),
            pltpu.VMEM((owned, *cells), f32),
            pltpu.VMEM((owned, 2, *cells), f32),
            pltpu.SemaphoreType.DMA((6,)),
        ],
        compiler_params=room(outgoing_size + 4 * modulus.size),
        name="pack",
    )(*(pltpu.with_memory_space_constraint(a, pltpu.HBM) for a in (send_list[0].T, brick_list, mod, fib)))
    arrived = lax.all_to_all(outgoing, "zone", split_axis=0, concat_axis=0, tiled=True)
    state = (K, SUBL, 2 * subzones, LANES)
    sites = K * SUBL * 2 * subzones
    table = (2 * LANES, 2 * LANES)
    start, sten0, neighbours = pl.pallas_call(
        prepare_kernel,
        out_shape=(shape(state, f32), shape(state, f32), shape(table, jnp.bfloat16)),
        in_specs=[VMEM],
        out_specs=(VMEM,) * 3,
        scratch_shapes=[pltpu.VMEM((sites, 2 * LANES), f32)],
        compiler_params=room(8 * seen.size),
        cost_estimate=pl.CostEstimate(flops=2**24, bytes_accessed=16 * seen.size, transcendentals=0),
        name="prepare",
    )(seen)
    slots = pl.pallas_call(
        solve_kernel,
        out_shape=shape((zones, lines, cap, 2, *cells), f32),
        in_specs=[VMEM, SMEM] + [VMEM] * 4,
        out_specs=VMEM,
        scratch_shapes=[
            pltpu.VMEM((3, sites, LANES), f32),
            pltpu.VMEM((SWEEPS - 1, *state), f32),
            pltpu.VMEM((SWEEPS, 2, *state), f32),
            pltpu.VMEM(state, f32),
            pltpu.VMEM((3, sites, LANES), f32),
            pltpu.VMEM((sites, 2 * LANES), f32),
            pltpu.VMEM((subzones, zones * rows, LANES), f32),
        ],
        compiler_params=room((8 * SWEEPS + 8) * seen.size + 2 * outgoing_size + (2 + subzones) * slot_size),
        name="solve",
    )(bricks, wave_sq, arrived.reshape(zones * rows, LANES), start, sten0, neighbours)
    slots = slots.reshape(zones * lines, cap, 2, *cells)
    mine = lax.all_to_all(slots, ("zone", "line"), split_axis=0, concat_axis=0, tiled=True)
    if cores == 2:
        other = lax.ppermute(mine, "core", [(0, 1), (1, 0)])
    else:
        other = jnp.zeros_like(mine)
    mine, other = (a.reshape(zones, lines, cap, 2, *cells) for a in (mine, other))
    whole = jax.ShapeDtypeStruct((owned, 3, *cells), f32)
    results = pl.pallas_call(
        functools.partial(update_kernel, float(lines * cores)),
        out_shape=(whole, whole, whole),
        in_specs=[VMEM] * 8,
        out_specs=(VMEM, VMEM, VMEM),
        scratch_shapes=[
            pltpu.VMEM((owned + 1, 2, *cells), f32),
            pltpu.VMEM((owned + 1, 1, LANES), f32),
        ],
        compiler_params=room(10 * modulus.size + outgoing_size + 2 * slot_size),
        name="update",
    )(send_table, mine, other, arrived, mod, first, second, fib)
    return tuple(r.reshape(modulus.shape) for r in results)


def solution(mesh):
    zones, freqs = mesh.shape["zone"], mesh.shape["freq"]
    cores = 2 if freqs % 2 == 0 else 1
    fine = Mesh(mesh.devices.reshape(zones, freqs // cores, cores), ("zone", "line", "core"))
    freq = ("line", "core")
    brick = P("zone", None, None, None)
    placed = (brick, brick, brick, P("zone", None, None), P(freq, "zone", None, None, None), P(freq), P("zone", None, None), P("zone", None))
    return jax.shard_map(on_device, mesh=fine, in_specs=placed, out_specs=(brick, brick, brick), check_vma=False)
```

```python
import functools

import jax
import jax.numpy as jnp
from jax import lax
from jax.experimental import pallas as pl
from jax.experimental.pallas import tpu as pltpu
from jax.sharding import Mesh, PartitionSpec as P

BZ = 32
K = 8
SWEEPS = 6
LANES = 128
SUBL = 8

relax_rate = 0.25
learn_rate = 0.1
beta_first = 0.9
beta_second = 0.99
smooth_rate = 0.5
adam_eps = 1e-08

VMEM = pl.BlockSpec(memory_space=pltpu.VMEM)
SMEM = pl.BlockSpec(memory_space=pltpu.SMEM)
HBM = pl.BlockSpec(memory_space=pltpu.HBM)


def room(words):
    return pltpu.CompilerParams(vmem_limit_bytes=4 * words + 2**21)


def pack_kernel(
    send_hbm, brick_hbm, modulus_hbm, fiber_hbm,
    out_ref, send_out, brick_out,
    send_ref, brick_ref, slot_ref, modulus_ref, fiber_ref, plane_ref, sems,
):
    pairs = (
        (send_hbm, send_ref), (brick_hbm, brick_ref), (modulus_hbm, modulus_ref), (fiber_hbm, fiber_ref),
        (send_hbm, send_out), (brick_hbm, slot_ref),
    )
    copies = [pltpu.make_async_copy(a, b, sems.at[i]) for i, (a, b) in enumerate(pairs)]
    for copy in copies:
        copy.start()
    for copy in copies[:4]:
        copy.wait()
    cap, zones = send_ref.shape
    pitch = out_ref.shape[0] // zones
    owned = modulus_ref.shape[0]
    for b in range(owned):
        fib = fiber_ref[b]
        base = modulus_ref[b, 0]
        plane_ref[b, 0] = base + (modulus_ref[b, 1] - base) * fib * fib
        plane_ref[b, 1] = modulus_ref[b, 2]
    slot_at = lax.broadcasted_iota(jnp.int32, (SUBL, LANES), 1)
    for first in range(0, zones * cap, LANES):
        uses = jnp.zeros((SUBL, LANES), jnp.float32)
        for s in range(brick_ref.shape[0]):
            for k in range(brick_ref.shape[1]):
                uses = uses + jnp.where(slot_at == brick_ref[s, k] - first, 1.0, 0.0)
        for q in range(first, min(first + LANES, zones * cap)):
            wide = jnp.broadcast_to(uses[:1, q - first : q - first + 1], (1, LANES))
            row = q // cap * pitch + 2 * SUBL * cap + q % cap
            out_ref[row : row + 1] = wide
    for d in range(zones):
        for c in range(cap):
            local = jnp.maximum(send_ref[c, d], 0)
            for p in range(2):
                row = d * pitch + (2 * c + p) * SUBL
                out_ref[row : row + SUBL] = plane_ref[local, p]
        row = 2 * SUBL * cap + cap
        if row < pitch:
            out_ref[d * pitch + row : (d + 1) * pitch] = jnp.zeros((pitch - row, LANES), jnp.float32)
    for copy in copies[4:]:
        copy.wait()
    slot = slot_ref[...]
    owner = jnp.zeros_like(slot)
    for d in range(1, zones):
        owner = owner + jnp.where(slot >= d * cap, 1, 0)
    brick_out[...] = owner * pitch + (slot - owner * cap) * (2 * SUBL)


def stencil(v, table_ref, res_ref):
    rows = v[0][0].shape[0]
    flat = jnp.concatenate([tile for line in v for tile in line], axis=0)
    high = flat.astype(jnp.bfloat16)
    low = (flat - high.astype(jnp.float32)).astype(jnp.bfloat16)
    res_ref[...] = jnp.dot(
        jnp.concatenate([high, low], axis=1), table_ref[...], preferred_element_type=jnp.float32
    )
    lane = lax.broadcasted_iota(jnp.int32, (rows, LANES), 1)
    low_half = lane < LANES // 2
    res = []
    for x, line in enumerate(v):
        res.append([])
        for y in range(len(line)):
            at = (x * len(line) + y) * rows
            below = res_ref[at - rows : at, LANES:] if y > 0 else 0.0
            above = res_ref[at + rows : at + 2 * rows, LANES:] if y + 1 < len(line) else 0.0
            total = res_ref[at : at + rows, :LANES] + jnp.where(low_half, below, above)
            sides = [v[i][y] for i in (x - 1, x + 1) if 0 <= i < len(v)]
            res[-1].append(total - sum(sides[1:], sides[0]))
    return res


def prepare_kernel(seen_ref, field_out, sten_out, table_out, res_ref):
    source = lax.broadcasted_iota(jnp.int32, table_out.shape, 0) % LANES
    column = lax.broadcasted_iota(jnp.int32, table_out.shape, 1)
    target = column % LANES
    step = jnp.abs(source - target)
    beside = jnp.logical_or(step == BZ, jnp.logical_and(step == 1, source // BZ == target // BZ))
    inner = jnp.where(step == 0, 6.0, jnp.where(beside, -1.0, 0.0))
    wrap = jnp.where(step == LANES - BZ, -1.0, 0.0)
    table_out[...] = jnp.where(column < LANES, inner, wrap).astype(table_out.dtype)
    lines, subl, rows, _ = field_out.shape
    subzones = rows // 2
    for x in range(lines):
        for y in range(subl):
            for p in range(2):
                at = p * subl * lines + y * lines + x
                field_out[x, y, p * subzones : (p + 1) * subzones] = seen_ref[
                    pl.ds(at, subzones, stride=2 * subl * lines), :
                ]
    sten = stencil([[field_out[x, y] for y in range(subl)] for x in range(lines)], table_out, res_ref)
    for x in range(lines):
        for y in range(subl):
            sten_out[x, y] = sten[x][y]


def solve_kernel(
    brick_ref, wave_ref, data_ref, start_ref, sten0_ref, table_ref, keep_ref, give_ref,
    coef_ref, field_ref, sten_ref, lam_ref, grad_ref, res_ref, sum_ref,
):
    subzones, entries = brick_ref.shape
    rows = 2 * subzones
    zones, cap = keep_ref.shape[:2]
    pitch = data_ref.shape[0] // zones
    core = lax.axis_index("core")
    wave = wave_ref[0]
    table = brick_ref[...]
    starts = [[pl.multiple_of(table[s, k], SUBL) for k in range(entries)] for s in range(subzones)]
    grid = [(x, y) for x in range(entries) for y in range(SUBL)]

    def swap(v):
        return pltpu.roll(v, subzones, 0)

    def moduli(s, k):
        return data_ref[pl.ds(starts[s][k], SUBL)], data_ref[pl.ds(starts[s][k] + SUBL, SUBL)]

    def rows_of(p, s, k):
        return pl.ds(k * SUBL * rows + p * subzones + s, SUBL, stride=rows)

    for s in range(subzones):
        for k in range(entries):
            shear, damping = moduli(s, k)
            rate = relax_rate / (6.0 * shear + wave)
            alpha = 1.0 + rate * wave
            beta = rate * shear
            gamma = beta * damping
            for p in range(2):
                coef_ref[0, rows_of(p, s, k), :] = alpha
                coef_ref[1, rows_of(p, s, k), :] = beta
                coef_ref[2, rows_of(p, s, k), :] = gamma if p == 0 else -gamma

    def coef(i, x, y):
        at = (x * SUBL + y) * rows
        return coef_ref[i, at : at + rows]

    def field(t, x, y):
        return field_ref[t - 1, x, y] if t > 0 else start_ref[x, y]

    for t in range(SWEEPS):
        if t == 0:
            sten = [[sten0_ref[x, y] for y in range(SUBL)] for x in range(entries)]
        else:
            sten = stencil([[field(t, x, y) for y in range(SUBL)] for x in range(entries)], table_ref, res_ref)
        for x, y in grid:
            own = sten[x][y]
            turned = swap(own)
            sten_ref[t, 0, x, y] = own
            sten_ref[t, 1, x, y] = turned
            new = coef(0, x, y) * field(t, x, y) - coef(1, x, y) * own + coef(2, x, y) * turned
            if t + 1 < SWEEPS:
                field_ref[t, x, y] = new
            else:
                lam_ref[x, y] = new - start_ref[x, y]

    for t in reversed(range(SWEEPS)):
        back = [[None] * SUBL for _ in range(entries)]
        for x, y in grid:
            lam = lam_ref[x, y]
            parts = (lam * field(t, x, y), lam * sten_ref[t, 0, x, y], lam * sten_ref[t, 1, x, y])
            at = (x * SUBL + y) * rows
            for i, part in enumerate(parts):
                if t + 1 < SWEEPS:
                    part = part + grad_ref[i, at : at + rows]
                grad_ref[i, at : at + rows] = part
            if t > 0:
                back[x][y] = coef(1, x, y) * lam + coef(2, x, y) * swap(lam)
        if t > 0:
            sten = stencil(back, table_ref, res_ref)
            for x, y in grid:
                lam_ref[x, y] = coef(0, x, y) * lam_ref[x, y] - sten[x][y]

    sum_ref[...] = jnp.zeros_like(sum_ref)
    for s in range(subzones):
        for k in range(entries):
            shear, damping = moduli(s, k)
            diag = 6.0 * shear + wave
            rate = relax_rate / diag
            real, imag = ([grad_ref[i, rows_of(p, s, k), :] for i in range(3)] for p in range(2))
            g_alpha, g_beta, g_gamma = real[0] + imag[0], real[1] + imag[1], real[2] - imag[2]
            mixed = damping * g_gamma - g_beta
            g_rate = wave * g_alpha + shear * mixed
            sum_ref[s, pl.ds(starts[s][k], SUBL)] += rate * (mixed - 6.0 * g_rate / diag)
            sum_ref[s, pl.ds(starts[s][k] + SUBL, SUBL)] += rate * shear * g_gamma
    for out_ref, half in ((keep_ref, core), (give_ref, 1 - core)):
        first = pl.multiple_of(half * (cap * SUBL), SUBL)
        for o in range(zones):
            for j in range(cap):
                at = pl.ds(first + (o * pitch + j * SUBL), SUBL)
                total = sum_ref[0, at]
                for s in range(1, subzones):
                    total = total + sum_ref[s, at]
                out_ref[o, j] = 2.0 * total


def join_kernel(keep_ref, given_ref, out_ref):
    total = keep_ref[...] + given_ref[...]
    for y in range(out_ref.shape[1]):
        out_ref[:, y] = total


def update_kernel(
    freq_count, send_ref, mine_ref, other_ref, data_ref, modulus_ref, first_ref, second_ref, fiber_ref,
    modulus_out, first_out, second_out, total_ref, use_ref,
):
    cap, zones = send_ref.shape
    owned = modulus_ref.shape[0]
    lane = lax.broadcasted_iota(jnp.int32, (SUBL, LANES), 1)
    z_first = lane % BZ == 0
    z_last = lane % BZ == BZ - 1
    table = send_ref[...]
    total_ref[...] = jnp.zeros_like(total_ref)
    use_ref[...] = jnp.zeros_like(use_ref)
    lower = lax.axis_index("core") == 0
    pitch = data_ref.shape[0] // zones
    for d in range(zones):
        units = [[], []]
        for j in range(cap):
            own, got = mine_ref[d, 0, j], other_ref[d, 0, j]
            for y in range(1, mine_ref.shape[1]):
                own, got = own + mine_ref[d, y, j], got + other_ref[d, y, j]
            units[0].append(jnp.where(lower, own, got))
            units[1].append(jnp.where(lower, got, own))
        units = units[0] + units[1]
        for c in range(cap):
            local = table[c, d]
            local = jnp.where(local < 0, owned, local)
            for p in range(2):
                total_ref[local, p] += units[2 * c + p]
            use_ref[local] += data_ref[pl.ds(d * pitch + 2 * SUBL * cap + c, 1)]
    for b in range(owned):
        fib = fiber_ref[b]
        fib_sq = fib * fib
        g_shear, g_damping = total_ref[b, 0], total_ref[b, 1]
        share = 1.0 / (freq_count * jnp.maximum(use_ref[b], 1.0))
        for p, grad in enumerate((g_shear * (1.0 - fib_sq), g_shear * fib_sq, g_damping)):
            descent = grad * share
            new_first = beta_first * first_ref[b, p] + (1.0 - beta_first) * descent
            new_second = beta_second * second_ref[b, p] + (1.0 - beta_second) * descent * descent
            stepped = modulus_ref[b, p] - learn_rate * new_first / (jnp.sqrt(new_second) + adam_eps)
            lower = jnp.where(z_first, stepped, pltpu.roll(stepped, 1, 1))
            upper = jnp.where(z_last, stepped, pltpu.roll(stepped, LANES - 1, 1))
            first_out[b, p] = new_first
            second_out[b, p] = new_second
            modulus_out[b, p] = stepped + smooth_rate * fib_sq * (0.5 * (lower + upper) - stepped)


def on_device(modulus, first_moment, second_moment, fiber, measured, wave_sq, send_list, brick_list):
    zones = lax.axis_size("zone")
    lines = lax.axis_size("line")
    cores = lax.axis_size("core")
    owned = modulus.shape[0]
    cells = (SUBL, LANES)
    cap = send_list.shape[2]
    subzones = brick_list.shape[0]
    planes = lambda a: a.reshape(owned, 3, *cells)
    mod, first, second = planes(modulus), planes(first_moment), planes(second_moment)
    fib = fiber.reshape(owned, *cells)
    seen = measured.reshape(subzones, 2, K, SUBL, LANES).swapaxes(2, 3).reshape(-1, LANES)
    f32 = jnp.float32
    rows = 2 * SUBL * cap + -(-cap // SUBL) * SUBL
    outgoing_size = zones * rows * LANES
    slot_size = zones * lines * cap * 2 * SUBL * LANES
    i32 = jnp.int32
    shape = jax.ShapeDtypeStruct
    outgoing, send_table, bricks = pl.pallas_call(
        pack_kernel,
        out_shape=(
            shape((zones * rows, LANES), f32), shape((cap, zones), i32), shape(brick_list.shape, i32),
        ),
        in_specs=[HBM] * 4,
        out_specs=(VMEM,) * 3,
        scratch_shapes=[
            pltpu.SMEM((cap, zones), i32),
            pltpu.SMEM(brick_list.shape, i32),
            pltpu.VMEM(brick_list.shape, i32),
            pltpu.VMEM((owned, 3, *cells), f32),
            pltpu.VMEM((owned, *cells), f32),
            pltpu.VMEM((owned, 2, *cells), f32),
            pltpu.SemaphoreType.DMA((6,)),
        ],
        compiler_params=room(outgoing_size + 4 * modulus.size),
        name="pack",
    )(*(pltpu.with_memory_space_constraint(a, pltpu.HBM) for a in (send_list[0].T, brick_list, mod, fib)))
    arrived = lax.all_to_all(outgoing, "zone", split_axis=0, concat_axis=0, tiled=True)
    state = (K, SUBL, 2 * subzones, LANES)
    sites = K * SUBL * 2 * subzones
    table = (2 * LANES, 2 * LANES)
    start, sten0, neighbours = pl.pallas_call(
        prepare_kernel,
        out_shape=(shape(state, f32), shape(state, f32), shape(table, jnp.bfloat16)),
        in_specs=[VMEM],
        out_specs=(VMEM,) * 3,
        scratch_shapes=[pltpu.VMEM((sites, 2 * LANES), f32)],
        compiler_params=room(8 * seen.size),
        cost_estimate=pl.CostEstimate(flops=2**24, bytes_accessed=16 * seen.size, transcendentals=0),
        name="prepare",
    )(seen)
    half = shape((zones, cap, *cells), f32)
    keep, give = pl.pallas_call(
        solve_kernel,
        out_shape=(half, half),
        in_specs=[VMEM, SMEM] + [VMEM] * 4,
        out_specs=(VMEM, VMEM),
        scratch_shapes=[
            pltpu.VMEM((3, sites, LANES), f32),
            pltpu.VMEM((SWEEPS - 1, *state), f32),
            pltpu.VMEM((SWEEPS, 2, *state), f32),
            pltpu.VMEM(state, f32),
            pltpu.VMEM((3, sites, LANES), f32),
            pltpu.VMEM((sites, 2 * LANES), f32),
            pltpu.VMEM((subzones, zones * rows, LANES), f32),
        ],
        compiler_params=room((8 * SWEEPS + 8) * seen.size + 2 * outgoing_size + (2 + subzones) * slot_size),
        name="solve",
    )(bricks, wave_sq, arrived, start, sten0, neighbours)
    other_core = [(0, 1), (1, 0)]
    slots = pl.pallas_call(
        join_kernel,
        out_shape=shape((zones, lines, cap, *cells), f32),
        in_specs=[VMEM, VMEM],
        out_specs=VMEM,
        compiler_params=room(2 * slot_size),
        name="join",
    )(keep, lax.ppermute(give, "core", other_core))
    slots = slots.reshape(zones * lines, cap, *cells)
    mine = lax.all_to_all(slots, ("zone", "line"), split_axis=0, concat_axis=0, tiled=True)
    other = lax.ppermute(mine, "core", other_core)
    mine, other = (a.reshape(zones, lines, cap, *cells) for a in (mine, other))
    whole = jax.ShapeDtypeStruct((owned, 3, *cells), f32)
    results = pl.pallas_call(
        functools.partial(update_kernel, float(lines * cores)),
        out_shape=(whole, whole, whole),
        in_specs=[VMEM] * 8,
        out_specs=(VMEM, VMEM, VMEM),
        scratch_shapes=[
            pltpu.VMEM((owned + 1, 2, *cells), f32),
            pltpu.VMEM((owned + 1, 1, LANES), f32),
        ],
        compiler_params=room(10 * modulus.size + outgoing_size + 2 * slot_size),
        name="update",
    )(send_table, mine, other, arrived, mod, first, second, fib)
    return tuple(r.reshape(modulus.shape) for r in results)


def solution(mesh):
    zones, freqs = mesh.shape["zone"], mesh.shape["freq"]
    cores = 2 if freqs % 2 == 0 else 1
    fine = Mesh(mesh.devices.reshape(zones, freqs // cores, cores), ("zone", "line", "core"))
    freq = ("line", "core")
    brick = P("zone", None, None, None)
    placed = (brick, brick, brick, P("zone", None, None), P(freq, "zone", None, None, None), P(freq), P("zone", None, None), P("zone", None))
    return jax.shard_map(on_device, mesh=fine, in_specs=placed, out_specs=(brick, brick, brick), check_vma=False)
```

```python
import functools

import jax
import jax.numpy as jnp
from jax import lax
from jax.experimental import pallas as pl
from jax.experimental.pallas import tpu as pltpu
from jax.sharding import Mesh, PartitionSpec as P

BZ = 32
K = 8
SWEEPS = 6
LANES = 128
SUBL = 8

relax_rate = 0.25
learn_rate = 0.1
beta_first = 0.9
beta_second = 0.99
smooth_rate = 0.5
adam_eps = 1e-08

VMEM = pl.BlockSpec(memory_space=pltpu.VMEM)
SMEM = pl.BlockSpec(memory_space=pltpu.SMEM)
HBM = pl.BlockSpec(memory_space=pltpu.HBM)


def room(words):
    return pltpu.CompilerParams(vmem_limit_bytes=4 * words + 2**21)


def pack_kernel(
    send_hbm, brick_hbm, modulus_hbm, fiber_hbm,
    out_ref, send_out, brick_out,
    send_ref, brick_ref, slot_ref, modulus_ref, fiber_ref, plane_ref, sems,
):
    pairs = (
        (send_hbm, send_ref), (brick_hbm, brick_ref), (modulus_hbm, modulus_ref), (fiber_hbm, fiber_ref),
        (send_hbm, send_out), (brick_hbm, slot_ref),
    )
    copies = [pltpu.make_async_copy(a, b, sems.at[i]) for i, (a, b) in enumerate(pairs)]
    for copy in copies:
        copy.start()
    for copy in copies[:4]:
        copy.wait()
    cap, zones = send_ref.shape
    pitch = out_ref.shape[0] // zones
    owned = modulus_ref.shape[0]
    for b in range(owned):
        fib = fiber_ref[b]
        base = modulus_ref[b, 0]
        plane_ref[b, 0] = base + (modulus_ref[b, 1] - base) * fib * fib
        plane_ref[b, 1] = modulus_ref[b, 2]
    slot_at = lax.broadcasted_iota(jnp.int32, (SUBL, LANES), 1)
    for first in range(0, zones * cap, LANES):
        uses = jnp.zeros((SUBL, LANES), jnp.float32)
        for s in range(brick_ref.shape[0]):
            for k in range(brick_ref.shape[1]):
                uses = uses + jnp.where(slot_at == brick_ref[s, k] - first, 1.0, 0.0)
        for q in range(first, min(first + LANES, zones * cap)):
            wide = jnp.broadcast_to(uses[:1, q - first : q - first + 1], (1, LANES))
            row = q // cap * pitch + 2 * SUBL * cap + q % cap
            out_ref[row : row + 1] = wide
    for d in range(zones):
        for c in range(cap):
            local = jnp.maximum(send_ref[c, d], 0)
            for p in range(2):
                row = d * pitch + (2 * c + p) * SUBL
                out_ref[row : row + SUBL] = plane_ref[local, p]
    for copy in copies[4:]:
        copy.wait()
    slot = slot_ref[...]
    owner = jnp.zeros_like(slot)
    for d in range(1, zones):
        owner = owner + jnp.where(slot >= d * cap, 1, 0)
    subzones = slot.shape[0]
    brick_out[:subzones] = owner * pitch + (slot - owner * cap) * (2 * SUBL)
    brick_out[subzones:] = slot * (2 * SUBL)


def stencil(v, table_ref, res_ref):
    rows = v[0][0].shape[0]
    flat = jnp.concatenate([tile for line in v for tile in line], axis=0)
    high = flat.astype(jnp.bfloat16)
    low = (flat - high.astype(jnp.float32)).astype(jnp.bfloat16)
    res_ref[...] = jnp.dot(
        jnp.concatenate([high, low], axis=1), table_ref[...], preferred_element_type=jnp.float32
    )
    lane = lax.broadcasted_iota(jnp.int32, (rows, LANES), 1)
    low_half = lane < LANES // 2
    res = []
    for x, line in enumerate(v):
        res.append([])
        for y in range(len(line)):
            at = (x * len(line) + y) * rows
            below = res_ref[at - rows : at, LANES:] if y > 0 else 0.0
            above = res_ref[at + rows : at + 2 * rows, LANES:] if y + 1 < len(line) else 0.0
            total = res_ref[at : at + rows, :LANES] + jnp.where(low_half, below, above)
            sides = [v[i][y] for i in (x - 1, x + 1) if 0 <= i < len(v)]
            res[-1].append(total - sum(sides[1:], sides[0]))
    return res


def prepare_kernel(seen_ref, field_out, sten_out, table_out, res_ref):
    source = lax.broadcasted_iota(jnp.int32, table_out.shape, 0) % LANES
    column = lax.broadcasted_iota(jnp.int32, table_out.shape, 1)
    target = column % LANES
    step = jnp.abs(source - target)
    beside = jnp.logical_or(step == BZ, jnp.logical_and(step == 1, source // BZ == target // BZ))
    inner = jnp.where(step == 0, 6.0, jnp.where(beside, -1.0, 0.0))
    wrap = jnp.where(step == LANES - BZ, -1.0, 0.0)
    table_out[...] = jnp.where(column < LANES, inner, wrap).astype(table_out.dtype)
    lines, subl, rows, _ = field_out.shape
    subzones = rows // 2
    for x in range(lines):
        for y in range(subl):
            for p in range(2):
                at = p * subl * lines + y * lines + x
                field_out[x, y, p * subzones : (p + 1) * subzones] = seen_ref[
                    pl.ds(at, subzones, stride=2 * subl * lines), :
                ]
    sten = stencil([[field_out[x, y] for y in range(subl)] for x in range(lines)], table_out, res_ref)
    for x in range(lines):
        for y in range(subl):
            sten_out[x, y] = sten[x][y]


def solve_kernel(
    brick_ref, wave_ref, data_ref, start_ref, sten0_ref, table_ref, keep_ref, give_ref,
    coef_ref, field_ref, sten_ref, lam_ref, grad_ref, res_ref, sum_ref,
):
    subzones, entries = brick_ref.shape[0] // 2, brick_ref.shape[1]
    rows = 2 * subzones
    zones, cap = keep_ref.shape[:2]
    core = lax.axis_index("core")
    wave = wave_ref[0]
    table = brick_ref[...]
    starts = [[table[s, k] for k in range(entries)] for s in range(subzones)]
    slots = [[pl.multiple_of(table[subzones + s, k], SUBL) for k in range(entries)] for s in range(subzones)]
    grid = [(x, y) for x in range(entries) for y in range(SUBL)]

    def swap(v):
        return pltpu.roll(v, subzones, 0)

    def moduli(s, k):
        return data_ref[pl.ds(starts[s][k], SUBL)], data_ref[pl.ds(starts[s][k] + SUBL, SUBL)]

    def rows_of(p, s, k):
        return pl.ds(k * SUBL * rows + p * subzones + s, SUBL, stride=rows)

    for s in range(subzones):
        for k in range(entries):
            shear, damping = moduli(s, k)
            rate = relax_rate / (6.0 * shear + wave)
            alpha = 1.0 + rate * wave
            beta = rate * shear
            gamma = beta * damping
            for p in range(2):
                coef_ref[0, rows_of(p, s, k), :] = alpha
                coef_ref[1, rows_of(p, s, k), :] = beta
                coef_ref[2, rows_of(p, s, k), :] = gamma if p == 0 else -gamma

    def coef(i, x, y):
        at = (x * SUBL + y) * rows
        return coef_ref[i, at : at + rows]

    def field(t, x, y):
        return field_ref[t - 1, x, y] if t > 0 else start_ref[x, y]

    for t in range(SWEEPS):
        if t == 0:
            sten = [[sten0_ref[x, y] for y in range(SUBL)] for x in range(entries)]
        else:
            sten = stencil([[field(t, x, y) for y in range(SUBL)] for x in range(entries)], table_ref, res_ref)
        for x, y in grid:
            own = sten[x][y]
            turned = swap(own)
            sten_ref[t, 0, x, y] = own
            sten_ref[t, 1, x, y] = turned
            new = coef(0, x, y) * field(t, x, y) - coef(1, x, y) * own + coef(2, x, y) * turned
            if t + 1 < SWEEPS:
                field_ref[t, x, y] = new
            else:
                lam_ref[x, y] = new - start_ref[x, y]

    for t in reversed(range(SWEEPS)):
        back = [[None] * SUBL for _ in range(entries)]
        for x, y in grid:
            lam = lam_ref[x, y]
            parts = (lam * field(t, x, y), lam * sten_ref[t, 0, x, y], lam * sten_ref[t, 1, x, y])
            at = (x * SUBL + y) * rows
            for i, part in enumerate(parts):
                if t + 1 < SWEEPS:
                    part = part + grad_ref[i, at : at + rows]
                grad_ref[i, at : at + rows] = part
            if t > 0:
                back[x][y] = coef(1, x, y) * lam + coef(2, x, y) * swap(lam)
        if t > 0:
            sten = stencil(back, table_ref, res_ref)
            for x, y in grid:
                lam_ref[x, y] = coef(0, x, y) * lam_ref[x, y] - sten[x][y]

    sum_ref[...] = jnp.zeros_like(sum_ref)
    for s in range(subzones):
        for k in range(entries):
            shear, damping = moduli(s, k)
            diag = 6.0 * shear + wave
            rate = relax_rate / diag
            real, imag = ([grad_ref[i, rows_of(p, s, k), :] for i in range(3)] for p in range(2))
            g_alpha, g_beta, g_gamma = real[0] + imag[0], real[1] + imag[1], real[2] - imag[2]
            mixed = damping * g_gamma - g_beta
            g_rate = wave * g_alpha + shear * mixed
            sum_ref[s, pl.ds(slots[s][k], SUBL)] += rate * (mixed - 6.0 * g_rate / diag)
            sum_ref[s, pl.ds(slots[s][k] + SUBL, SUBL)] += rate * shear * g_gamma
    for out_ref, half in ((keep_ref, core), (give_ref, 1 - core)):
        first = pl.multiple_of(half * (cap * SUBL), SUBL)
        for o in range(zones):
            for j in range(cap):
                at = pl.ds(first + (o * 2 * cap + j) * SUBL, SUBL)
                total = sum_ref[0, at]
                for s in range(1, subzones):
                    total = total + sum_ref[s, at]
                out_ref[o, j] = 2.0 * total


def join_kernel(keep_ref, given_ref, out_ref):
    total = keep_ref[...] + given_ref[...]
    for y in range(out_ref.shape[1]):
        out_ref[:, y] = total


def update_kernel(
    freq_count, send_ref, mine_ref, other_ref, data_ref, modulus_ref, first_ref, second_ref, fiber_ref,
    modulus_out, first_out, second_out, total_ref, use_ref,
):
    cap, zones = send_ref.shape
    owned = modulus_ref.shape[0]
    lots = total_ref.shape[0]
    lane = lax.broadcasted_iota(jnp.int32, (SUBL, LANES), 1)
    z_first = lane % BZ == 0
    z_last = lane % BZ == BZ - 1
    table = send_ref[...]
    total_ref[...] = jnp.zeros_like(total_ref)
    use_ref[...] = jnp.zeros_like(use_ref)
    lower = lax.axis_index("core") == 0
    pitch = data_ref.shape[0] // zones
    for d in range(zones):
        units = [[], []]
        for j in range(cap):
            own, got = mine_ref[d, 0, j], other_ref[d, 0, j]
            for y in range(1, mine_ref.shape[1]):
                own, got = own + mine_ref[d, y, j], got + other_ref[d, y, j]
            units[0].append(jnp.where(lower, own, got))
            units[1].append(jnp.where(lower, got, own))
        units = units[0] + units[1]
        for c in range(cap):
            local = table[c, d]
            local = jnp.where(local < 0, owned, local)
            lot = d % lots
            for p in range(2):
                total_ref[lot, c, local, p] += units[2 * c + p]
            use_ref[lot, c, local] += data_ref[pl.ds(d * pitch + 2 * SUBL * cap + c, 1)]
    for b in range(owned):
        fib = fiber_ref[b]
        fib_sq = fib * fib
        g_shear, g_damping = (sum(total_ref[i, c, b, p] for i in range(lots) for c in range(cap)) for p in range(2))
        uses = sum(use_ref[i, c, b] for i in range(lots) for c in range(cap))
        share = 1.0 / (freq_count * jnp.maximum(uses, 1.0))
        for p, grad in enumerate((g_shear * (1.0 - fib_sq), g_shear * fib_sq, g_damping)):
            descent = grad * share
            new_first = beta_first * first_ref[b, p] + (1.0 - beta_first) * descent
            new_second = beta_second * second_ref[b, p] + (1.0 - beta_second) * descent * descent
            stepped = modulus_ref[b, p] - learn_rate * new_first / (jnp.sqrt(new_second) + adam_eps)
            lower = jnp.where(z_first, stepped, pltpu.roll(stepped, 1, 1))
            upper = jnp.where(z_last, stepped, pltpu.roll(stepped, LANES - 1, 1))
            first_out[b, p] = new_first
            second_out[b, p] = new_second
            modulus_out[b, p] = stepped + smooth_rate * fib_sq * (0.5 * (lower + upper) - stepped)


def on_device(modulus, first_moment, second_moment, fiber, measured, wave_sq, send_list, brick_list):
    zones = lax.axis_size("zone")
    lines = lax.axis_size("line")
    cores = lax.axis_size("core")
    owned = modulus.shape[0]
    cells = (SUBL, LANES)
    cap = send_list.shape[2]
    subzones = brick_list.shape[0]
    planes = lambda a: a.reshape(owned, 3, *cells)
    mod, first, second = planes(modulus), planes(first_moment), planes(second_moment)
    fib = fiber.reshape(owned, *cells)
    seen = measured.reshape(subzones, 2, K, SUBL, LANES).swapaxes(2, 3).reshape(-1, LANES)
    f32 = jnp.float32
    rows = 2 * SUBL * cap + cap
    outgoing_size = zones * rows * LANES
    slot_size = zones * lines * cap * 2 * SUBL * LANES
    i32 = jnp.int32
    shape = jax.ShapeDtypeStruct
    outgoing, send_table, bricks = pl.pallas_call(
        pack_kernel,
        out_shape=(
            shape((zones * rows, LANES), f32), shape((cap, zones), i32), shape((2 * subzones, K), i32),
        ),
        in_specs=[HBM] * 4,
        out_specs=(VMEM,) * 3,
        scratch_shapes=[
            pltpu.SMEM((cap, zones), i32),
            pltpu.SMEM(brick_list.shape, i32),
            pltpu.VMEM(brick_list.shape, i32),
            pltpu.VMEM((owned, 3, *cells), f32),
            pltpu.VMEM((owned, *cells), f32),
            pltpu.VMEM((owned, 2, *cells), f32),
            pltpu.SemaphoreType.DMA((6,)),
        ],
        compiler_params=room(outgoing_size + 4 * modulus.size),
        name="pack",
    )(*(pltpu.with_memory_space_constraint(a, pltpu.HBM) for a in (send_list[0].T, brick_list, mod, fib)))
    outgoing = outgoing.reshape(zones * rows, 1, LANES)
    arrived = lax.all_to_all(outgoing, "zone", split_axis=0, concat_axis=0, tiled=True).reshape(zones * rows, LANES)
    state = (K, SUBL, 2 * subzones, LANES)
    sites = K * SUBL * 2 * subzones
    table = (2 * LANES, 2 * LANES)
    start, sten0, neighbours = pl.pallas_call(
        prepare_kernel,
        out_shape=(shape(state, f32), shape(state, f32), shape(table, jnp.bfloat16)),
        in_specs=[VMEM],
        out_specs=(VMEM,) * 3,
        scratch_shapes=[pltpu.VMEM((sites, 2 * LANES), f32)],
        compiler_params=room(8 * seen.size),
        cost_estimate=pl.CostEstimate(flops=2**24, bytes_accessed=16 * seen.size, transcendentals=0),
        name="prepare",
    )(seen)
    half = shape((zones, cap, *cells), f32)
    keep, give = pl.pallas_call(
        solve_kernel,
        out_shape=(half, half),
        in_specs=[VMEM, SMEM] + [VMEM] * 4,
        out_specs=(VMEM, VMEM),
        scratch_shapes=[
            pltpu.VMEM((3, sites, LANES), f32),
            pltpu.VMEM((SWEEPS - 1, *state), f32),
            pltpu.VMEM((SWEEPS, 2, *state), f32),
            pltpu.VMEM(state, f32),
            pltpu.VMEM((3, sites, LANES), f32),
            pltpu.VMEM((sites, 2 * LANES), f32),
            pltpu.VMEM((subzones, zones * cap * 2 * SUBL, LANES), f32),
        ],
        compiler_params=room((8 * SWEEPS + 8) * seen.size + 2 * outgoing_size + (2 + subzones) * slot_size),
        name="solve",
    )(bricks, wave_sq, arrived, start, sten0, neighbours)
    other_core = [(0, 1), (1, 0)]
    slots = pl.pallas_call(
        join_kernel,
        out_shape=shape((zones, lines, cap, *cells), f32),
        in_specs=[VMEM, VMEM],
        out_specs=VMEM,
        compiler_params=room(2 * slot_size),
        name="join",
    )(keep, lax.ppermute(give, "core", other_core))
    slots = slots.reshape(zones * lines, cap, *cells)
    mine = lax.all_to_all(slots, ("zone", "line"), split_axis=0, concat_axis=0, tiled=True)
    other = lax.ppermute(mine, "core", other_core)
    mine, other = (a.reshape(zones, lines, cap, *cells) for a in (mine, other))
    whole = jax.ShapeDtypeStruct((owned, 3, *cells), f32)
    results = pl.pallas_call(
        functools.partial(update_kernel, float(lines * cores)),
        out_shape=(whole, whole, whole),
        in_specs=[VMEM] * 8,
        out_specs=(VMEM, VMEM, VMEM),
        scratch_shapes=[
            pltpu.VMEM((2, cap, owned + 1, 2, *cells), f32),
            pltpu.VMEM((2, cap, owned + 1, 1, LANES), f32),
        ],
        compiler_params=room(10 * modulus.size + outgoing_size + 2 * slot_size),
        name="update",
    )(send_table, mine, other, arrived, mod, first, second, fib)
    return tuple(r.reshape(modulus.shape) for r in results)


def solution(mesh):
    zones, freqs = mesh.shape["zone"], mesh.shape["freq"]
    cores = 2 if freqs % 2 == 0 else 1
    fine = Mesh(mesh.devices.reshape(zones, freqs // cores, cores), ("zone", "line", "core"))
    freq = ("line", "core")
    brick = P("zone", None, None, None)
    placed = (brick, brick, brick, P("zone", None, None), P(freq, "zone", None, None, None), P(freq), P("zone", None, None), P("zone", None))
    return jax.shard_map(on_device, mesh=fine, in_specs=placed, out_specs=(brick, brick, brick), check_vma=False)
```

```python
import functools

import jax
import jax.numpy as jnp
from jax import lax
from jax.experimental import pallas as pl
from jax.experimental.pallas import tpu as pltpu
from jax.sharding import Mesh, PartitionSpec as P

BZ = 32
K = 8
SWEEPS = 6
LANES = 128
SUBL = 8

relax_rate = 0.25
learn_rate = 0.1
beta_first = 0.9
beta_second = 0.99
smooth_rate = 0.5
adam_eps = 1e-08

VMEM = pl.BlockSpec(memory_space=pltpu.VMEM)
SMEM = pl.BlockSpec(memory_space=pltpu.SMEM)
HBM = pl.BlockSpec(memory_space=pltpu.HBM)


def room(words):
    return pltpu.CompilerParams(vmem_limit_bytes=4 * words + 2**21)


def pack_kernel(
    send_hbm, brick_hbm, modulus_hbm, fiber_hbm,
    out_ref, send_out, brick_out,
    send_ref, brick_ref, slot_ref, modulus_ref, fiber_ref, plane_ref, sems,
):
    pairs = (
        (send_hbm, send_ref), (brick_hbm, brick_ref), (modulus_hbm, modulus_ref), (fiber_hbm, fiber_ref),
        (send_hbm, send_out), (brick_hbm, slot_ref),
    )
    copies = [pltpu.make_async_copy(a, b, sems.at[i]) for i, (a, b) in enumerate(pairs)]
    for copy in copies:
        copy.start()
    for copy in copies[:4]:
        copy.wait()
    cap, zones = send_ref.shape
    pitch = out_ref.shape[0] // zones
    owned = modulus_ref.shape[0]
    for b in range(owned):
        fib = fiber_ref[b]
        base = modulus_ref[b, 0]
        plane_ref[b, 0] = base + (modulus_ref[b, 1] - base) * fib * fib
        plane_ref[b, 1] = modulus_ref[b, 2]
    slot_at = lax.broadcasted_iota(jnp.int32, (SUBL, LANES), 1)
    for first in range(0, zones * cap, LANES):
        uses = jnp.zeros((SUBL, LANES), jnp.float32)
        for s in range(brick_ref.shape[0]):
            for k in range(brick_ref.shape[1]):
                uses = uses + jnp.where(slot_at == brick_ref[s, k] - first, 1.0, 0.0)
        for q in range(first, min(first + LANES, zones * cap)):
            wide = jnp.broadcast_to(uses[:1, q - first : q - first + 1], (1, LANES))
            row = q // cap * pitch + 2 * SUBL * cap + q % cap
            out_ref[row : row + 1] = wide
    for d in range(zones):
        for c in range(cap):
            local = jnp.maximum(send_ref[c, d], 0)
            for p in range(2):
                row = d * pitch + (2 * c + p) * SUBL
                out_ref[row : row + SUBL] = plane_ref[local, p]
    for copy in copies[4:]:
        copy.wait()
    slot = slot_ref[...]
    owner = jnp.zeros_like(slot)
    for d in range(1, zones):
        owner = owner + jnp.where(slot >= d * cap, 1, 0)
    subzones = slot.shape[0]
    brick_out[:subzones] = owner * pitch + (slot - owner * cap) * (2 * SUBL)
    brick_out[subzones:] = slot * (2 * SUBL)


def stencil(v, table_ref, res_ref):
    rows = v[0][0].shape[0]
    flat = jnp.concatenate([tile for line in v for tile in line], axis=0)
    high = flat.astype(jnp.bfloat16)
    low = (flat - high.astype(jnp.float32)).astype(jnp.bfloat16)
    res_ref[...] = jnp.dot(
        jnp.concatenate([high, low], axis=1), table_ref[...], preferred_element_type=jnp.float32
    )
    lane = lax.broadcasted_iota(jnp.int32, (rows, LANES), 1)
    low_half = lane < LANES // 2
    res = []
    for x, line in enumerate(v):
        res.append([])
        for y in range(len(line)):
            at = (x * len(line) + y) * rows
            below = res_ref[at - rows : at, LANES:] if y > 0 else 0.0
            above = res_ref[at + rows : at + 2 * rows, LANES:] if y + 1 < len(line) else 0.0
            total = res_ref[at : at + rows, :LANES] + jnp.where(low_half, below, above)
            sides = [v[i][y] for i in (x - 1, x + 1) if 0 <= i < len(v)]
            res[-1].append(total - sum(sides[1:], sides[0]))
    return res


def prepare(seen_ref, field_out, sten_out, table_out, res_ref):
    source = lax.broadcasted_iota(jnp.int32, table_out.shape, 0) % LANES
    column = lax.broadcasted_iota(jnp.int32, table_out.shape, 1)
    target = column % LANES
    step = jnp.abs(source - target)
    beside = jnp.logical_or(step == BZ, jnp.logical_and(step == 1, source // BZ == target // BZ))
    inner = jnp.where(step == 0, 6.0, jnp.where(beside, -1.0, 0.0))
    wrap = jnp.where(step == LANES - BZ, -1.0, 0.0)
    table_out[...] = jnp.where(column < LANES, inner, wrap).astype(table_out.dtype)
    lines, subl, rows, _ = field_out.shape
    subzones = rows // 2
    for x in range(lines):
        for y in range(subl):
            for p in range(2):
                at = p * subl * lines + y * lines + x
                field_out[x, y, p * subzones : (p + 1) * subzones] = seen_ref[
                    pl.ds(at, subzones, stride=2 * subl * lines), :
                ]
    sten = stencil([[field_out[x, y] for y in range(subl)] for x in range(lines)], table_out, res_ref)
    for x in range(lines):
        for y in range(subl):
            sten_out[x, y] = sten[x][y]


def solve_kernel(
    brick_ref, wave_ref, data_ref, seen_ref, keep_ref, give_ref,
    start_ref, sten0_ref, table_ref, coef_ref, field_ref, sten_ref, lam_ref, grad_ref, res_ref, sum_ref,
):
    subzones, entries = brick_ref.shape[0] // 2, brick_ref.shape[1]
    rows = 2 * subzones
    zones, cap = keep_ref.shape[:2]
    core = lax.axis_index("core")
    wave = jnp.broadcast_to(wave_ref[:, :1], (SUBL, LANES))
    table = brick_ref[...]
    starts = [[table[s, k] for k in range(entries)] for s in range(subzones)]
    slots = [[pl.multiple_of(table[subzones + s, k], SUBL) for k in range(entries)] for s in range(subzones)]
    prepare(seen_ref, start_ref, sten0_ref, table_ref, res_ref)
    grid = [(x, y) for x in range(entries) for y in range(SUBL)]

    def swap(v):
        return pltpu.roll(v, subzones, 0)

    def moduli(s, k):
        return data_ref[pl.ds(starts[s][k], SUBL)], data_ref[pl.ds(starts[s][k] + SUBL, SUBL)]

    def rows_of(p, s, k):
        return pl.ds(k * SUBL * rows + p * subzones + s, SUBL, stride=rows)

    for s in range(subzones):
        for k in range(entries):
            shear, damping = moduli(s, k)
            rate = relax_rate / (6.0 * shear + wave)
            alpha = 1.0 + rate * wave
            beta = rate * shear
            gamma = beta * damping
            for p in range(2):
                coef_ref[0, rows_of(p, s, k), :] = alpha
                coef_ref[1, rows_of(p, s, k), :] = beta
                coef_ref[2, rows_of(p, s, k), :] = gamma if p == 0 else -gamma

    def coef(i, x, y):
        at = (x * SUBL + y) * rows
        return coef_ref[i, at : at + rows]

    def field(t, x, y):
        return field_ref[t - 1, x, y] if t > 0 else start_ref[x, y]

    for t in range(SWEEPS):
        if t == 0:
            sten = [[sten0_ref[x, y] for y in range(SUBL)] for x in range(entries)]
        else:
            sten = stencil([[field(t, x, y) for y in range(SUBL)] for x in range(entries)], table_ref, res_ref)
        for x, y in grid:
            own = sten[x][y]
            turned = swap(own)
            sten_ref[t, 0, x, y] = own
            sten_ref[t, 1, x, y] = turned
            new = coef(0, x, y) * field(t, x, y) - coef(1, x, y) * own + coef(2, x, y) * turned
            if t + 1 < SWEEPS:
                field_ref[t, x, y] = new
            else:
                lam_ref[x, y] = new - start_ref[x, y]

    for t in reversed(range(SWEEPS)):
        back = [[None] * SUBL for _ in range(entries)]
        for x, y in grid:
            lam = lam_ref[x, y]
            parts = (lam * field(t, x, y), lam * sten_ref[t, 0, x, y], lam * sten_ref[t, 1, x, y])
            at = (x * SUBL + y) * rows
            for i, part in enumerate(parts):
                if t + 1 < SWEEPS:
                    part = part + grad_ref[i, at : at + rows]
                grad_ref[i, at : at + rows] = part
            if t > 0:
                back[x][y] = coef(1, x, y) * lam + coef(2, x, y) * swap(lam)
        if t > 0:
            sten = stencil(back, table_ref, res_ref)
            for x, y in grid:
                lam_ref[x, y] = coef(0, x, y) * lam_ref[x, y] - sten[x][y]

    sum_ref[...] = jnp.zeros_like(sum_ref)
    for s in range(subzones):
        for k in range(entries):
            shear, damping = moduli(s, k)
            diag = 6.0 * shear + wave
            rate = relax_rate / diag
            real, imag = ([grad_ref[i, rows_of(p, s, k), :] for i in range(3)] for p in range(2))
            g_alpha, g_beta, g_gamma = real[0] + imag[0], real[1] + imag[1], real[2] - imag[2]
            mixed = damping * g_gamma - g_beta
            g_rate = wave * g_alpha + shear * mixed
            sum_ref[s, pl.ds(slots[s][k], SUBL)] += rate * (mixed - 6.0 * g_rate / diag)
            sum_ref[s, pl.ds(slots[s][k] + SUBL, SUBL)] += rate * shear * g_gamma
    for out_ref, half in ((keep_ref, core), (give_ref, 1 - core)):
        first = pl.multiple_of(half * (cap * SUBL), SUBL)
        for o in range(zones):
            for j in range(cap):
                at = pl.ds(first + (o * 2 * cap + j) * SUBL, SUBL)
                total = sum_ref[0, at]
                for s in range(1, subzones):
                    total = total + sum_ref[s, at]
                out_ref[o, j] = 2.0 * total


def join_kernel(keep_ref, given_ref, out_ref):
    total = keep_ref[...] + given_ref[...]
    for y in range(out_ref.shape[1]):
        out_ref[:, y] = total


def update_kernel(
    freq_count, send_ref, mine_ref, other_ref, data_ref, modulus_ref, first_ref, second_ref, fiber_ref,
    modulus_out, first_out, second_out, total_ref, use_ref,
):
    cap, zones = send_ref.shape
    owned = modulus_ref.shape[0]
    lots = total_ref.shape[0]
    lane = lax.broadcasted_iota(jnp.int32, (SUBL, LANES), 1)
    z_first = lane % BZ == 0
    z_last = lane % BZ == BZ - 1
    table = send_ref[...]
    total_ref[...] = jnp.zeros_like(total_ref)
    use_ref[...] = jnp.zeros_like(use_ref)
    lower = lax.axis_index("core") == 0
    pitch = data_ref.shape[0] // zones
    for d in range(zones):
        units = [[], []]
        for j in range(cap):
            own, got = mine_ref[d, 0, j], other_ref[d, 0, j]
            for y in range(1, mine_ref.shape[1]):
                own, got = own + mine_ref[d, y, j], got + other_ref[d, y, j]
            units[0].append(jnp.where(lower, own, got))
            units[1].append(jnp.where(lower, got, own))
        units = units[0] + units[1]
        for c in range(cap):
            local = table[c, d]
            local = jnp.where(local < 0, owned, local)
            lot = d % lots
            for p in range(2):
                total_ref[lot, c, local, p] += units[2 * c + p]
            use_ref[lot, c, local] += data_ref[pl.ds(d * pitch + 2 * SUBL * cap + c, 1)]
    for b in range(owned):
        fib = fiber_ref[b]
        fib_sq = fib * fib
        g_shear, g_damping = (sum(total_ref[i, c, b, p] for i in range(lots) for c in range(cap)) for p in range(2))
        uses = sum(use_ref[i, c, b] for i in range(lots) for c in range(cap))
        share = 1.0 / (freq_count * jnp.maximum(uses, 1.0))
        for p, grad in enumerate((g_shear * (1.0 - fib_sq), g_shear * fib_sq, g_damping)):
            descent = grad * share
            new_first = beta_first * first_ref[b, p] + (1.0 - beta_first) * descent
            new_second = beta_second * second_ref[b, p] + (1.0 - beta_second) * descent * descent
            stepped = modulus_ref[b, p] - learn_rate * new_first / (jnp.sqrt(new_second) + adam_eps)
            lower = jnp.where(z_first, stepped, pltpu.roll(stepped, 1, 1))
            upper = jnp.where(z_last, stepped, pltpu.roll(stepped, LANES - 1, 1))
            first_out[b, p] = new_first
            second_out[b, p] = new_second
            modulus_out[b, p] = stepped + smooth_rate * fib_sq * (0.5 * (lower + upper) - stepped)


def on_device(modulus, first_moment, second_moment, fiber, measured, wave_sq, send_list, brick_list):
    zones = lax.axis_size("zone")
    lines = lax.axis_size("line")
    cores = lax.axis_size("core")
    owned = modulus.shape[0]
    cells = (SUBL, LANES)
    cap = send_list.shape[2]
    subzones = brick_list.shape[0]
    planes = lambda a: a.reshape(owned, 3, *cells)
    mod, first, second = planes(modulus), planes(first_moment), planes(second_moment)
    fib = fiber.reshape(owned, *cells)
    seen = measured.reshape(subzones, 2, K, SUBL, LANES).swapaxes(2, 3).reshape(-1, LANES)
    f32 = jnp.float32
    rows = 2 * SUBL * cap + cap
    outgoing_size = zones * rows * LANES
    slot_size = zones * lines * cap * 2 * SUBL * LANES
    i32 = jnp.int32
    shape = jax.ShapeDtypeStruct
    outgoing, send_table, bricks = pl.pallas_call(
        pack_kernel,
        out_shape=(
            shape((zones * rows, LANES), f32), shape((cap, zones), i32), shape((2 * subzones, K), i32),
        ),
        in_specs=[HBM] * 4,
        out_specs=(VMEM,) * 3,
        scratch_shapes=[
            pltpu.SMEM((cap, zones), i32),
            pltpu.SMEM(brick_list.shape, i32),
            pltpu.VMEM(brick_list.shape, i32),
            pltpu.VMEM((owned, 3, *cells), f32),
            pltpu.VMEM((owned, *cells), f32),
            pltpu.VMEM((owned, 2, *cells), f32),
            pltpu.SemaphoreType.DMA((6,)),
        ],
        compiler_params=room(outgoing_size + 4 * modulus.size),
        name="pack",
    )(*(pltpu.with_memory_space_constraint(a, pltpu.HBM) for a in (send_list[0].T, brick_list, mod, fib)))
    wave = lax.pad(wave_sq, f32(0), ((0, LANES - 1, 0),))[None]
    outgoing, wave = lax.optimization_barrier((outgoing, wave))
    outgoing = outgoing.reshape(zones * rows, 1, LANES)
    arrived = lax.all_to_all(outgoing, "zone", split_axis=0, concat_axis=0, tiled=True).reshape(zones * rows, LANES)
    state = (K, SUBL, 2 * subzones, LANES)
    sites = K * SUBL * 2 * subzones
    table = (2 * LANES, 2 * LANES)
    half = shape((zones, cap, *cells), f32)
    keep, give = pl.pallas_call(
        solve_kernel,
        out_shape=(half, half),
        in_specs=[VMEM] * 4,
        out_specs=(VMEM, VMEM),
        scratch_shapes=[
            pltpu.VMEM(state, f32),
            pltpu.VMEM(state, f32),
            pltpu.VMEM(table, jnp.bfloat16),
            pltpu.VMEM((3, sites, LANES), f32),
            pltpu.VMEM((SWEEPS - 1, *state), f32),
            pltpu.VMEM((SWEEPS, 2, *state), f32),
            pltpu.VMEM(state, f32),
            pltpu.VMEM((3, sites, LANES), f32),
            pltpu.VMEM((sites, 2 * LANES), f32),
            pltpu.VMEM((subzones, zones * cap * 2 * SUBL, LANES), f32),
        ],
        compiler_params=room((8 * SWEEPS + 11) * seen.size + 2 * outgoing_size + (2 + subzones) * slot_size),
        name="solve",
    )(bricks, wave, arrived, seen)
    other_core = [(0, 1), (1, 0)]
    slots = pl.pallas_call(
        join_kernel,
        out_shape=shape((zones, lines, cap, *cells), f32),
        in_specs=[VMEM, VMEM],
        out_specs=VMEM,
        compiler_params=room(2 * slot_size),
        name="join",
    )(keep, lax.ppermute(give, "core", other_core))
    slots = slots.reshape(zones * lines, cap, *cells)
    mine = lax.all_to_all(slots, ("zone", "line"), split_axis=0, concat_axis=0, tiled=True)
    other = lax.ppermute(mine, "core", other_core)
    mine, other = (a.reshape(zones, lines, cap, *cells) for a in (mine, other))
    whole = jax.ShapeDtypeStruct((owned, 3, *cells), f32)
    results = pl.pallas_call(
        functools.partial(update_kernel, float(lines * cores)),
        out_shape=(whole, whole, whole),
        in_specs=[VMEM] * 8,
        out_specs=(VMEM, VMEM, VMEM),
        scratch_shapes=[
            pltpu.VMEM((2, cap, owned + 1, 2, *cells), f32),
            pltpu.VMEM((2, cap, owned + 1, 1, LANES), f32),
        ],
        compiler_params=room(10 * modulus.size + outgoing_size + 2 * slot_size),
        name="update",
    )(send_table, mine, other, arrived, mod, first, second, fib)
    return tuple(r.reshape(modulus.shape) for r in results)


def solution(mesh):
    zones, freqs = mesh.shape["zone"], mesh.shape["freq"]
    cores = 2 if freqs % 2 == 0 else 1
    fine = Mesh(mesh.devices.reshape(zones, freqs // cores, cores), ("zone", "line", "core"))
    freq = ("line", "core")
    brick = P("zone", None, None, None)
    placed = (brick, brick, brick, P("zone", None, None), P(freq, "zone", None, None, None), P(freq), P("zone", None, None), P("zone", None))
    return jax.shard_map(on_device, mesh=fine, in_specs=placed, out_specs=(brick, brick, brick), check_vma=False)
```
